32 devices in a mesh: dp: 8 (over z, y), tensor: 4 (over x, core).
Axes of the slice: x: 2, y: 2, z: 4, core: 2. Of those that a mesh axis runs over, the one named last changes fastest.
Arguments:
- sampled_earlier_tokens: int32 [32, 169], P('dp'), may hold values from 0 to 4095
- quantizer_vectors: float32 [4096, 32], replicated, may hold values from -6 to 6
- summed_latent_canvas: float32 [32, 256, 32], P('dp'), may hold values from -6 to 6
- latent_lift_matrix: float32 [32, 1536], replicated, may hold values from -1 to 1
- location_tier_offset: float32 [256, 1536], replicated, may hold values from -3 to 3
- adaptive_norm_factors: float32 [1, 32, 6, 1536], P(None, 'dp'), may hold values from -3 to 3
- logit_sharpness: float32 [1, 16], P(None, 'tensor'), may hold values from 2 to 240, as said below
- probe_match_content_matrix: bfloat16 [1, 1536, 3, 1536], P(None, 'dp', None, 'tensor'), may hold values from -1 to 1, as said below
- mixing_projection_matrix: bfloat16 [1, 1536, 1536], P(None, 'tensor', 'dp'), may hold values from -0.15625 to 0.15625
- widening_projection_matrix: bfloat16 [1, 1536, 6144], P(None, 'dp', 'tensor'), may hold values from -0.15625 to 0.15625
- narrowing_projection_matrix: bfloat16 [1, 6144, 1536], P(None, 'tensor', 'dp'), may hold values from -0.078125 to 0.078125
- cached_lower_grid_lookups: bfloat16 [1, 32, 424, 1536], P(None, 'dp', None, 'tensor'), may hold values from -6 to 6
- cached_lower_grid_payloads: bfloat16 [1, 32, 424, 1536], P(None, 'dp', None, 'tensor'), may hold values from -6 to 6
- final_norm_factors: float32 [32, 2, 1536], P('dp'), may hold values from -3 to 3
- vocabulary_logit_matrix: bfloat16 [1536, 4096], P(None, 'tensor'), may hold values from -0.15625 to 0.15625
Outputs:
- logits: bfloat16 [32, 256, 4096], P('dp', None, 'tensor')
- canvas: float32 [32, 256, 32], P('dp')
The draws below stay inside these ranges and needn't reach their ends.
Inputs may be any that keep to these rules, and one draw needn't show every extreme that they name: `logit_sharpness`: Positive. `probe_match_content_matrix`: entries of spread about 1536 ** -0.5.
All inputs are finite; a program needn't handle non-finite values.
Results may differ from the reference program's by a relative error of at most 0.015.
Values may be sent and summed in bfloat16 or wider, within the bound.
A program may use at most 128 MiB of HBM per device.

```python
import math
import jax
import jax.numpy as jnp
from jax import lax

D = 1536
HEADS = 16
HDIM = 96
FF = 6144
VOCAB = 4096
CVAE = 32
LAYERS = 1
SIDE = 16
PREV = 13
CACHE = 424
TOK = 256
PREVTOK = 169
IMAGES = 32
N_TENSOR = 4


def draw_probe_match_content_matrix(key, part):
    base_draw = jax.random.truncated_normal(jax.random.fold_in(key, 11), -6.0, 6.0, (LAYERS, D, 3, D), jnp.float32) * D ** (-0.5)
    drawn_values = base_draw
    return drawn_values.astype(jnp.bfloat16)


def draw_logit_sharpness(key, part):
    exponent = jax.random.uniform(jax.random.fold_in(key, 23), (LAYERS, HEADS), jnp.float32, math.log(2.0), math.log(60.0))
    drawn_values = jnp.exp(exponent)
    return drawn_values


def plant(array, stream_key, least, top_value):
    extent = array.shape
    place = [jax.random.randint(jax.random.fold_in(stream_key, axis), (), 0, extent[axis]) for axis in range(len(extent))]
    array = array.at[tuple(place)].set(least)
    longest = extent.index(max(extent))
    place[longest] = (place[longest] + 1) % extent[longest]
    return array.at[tuple(place)].set(top_value)


def block_levels(key, dims, pieces, smallest, largest):
    factor_of = 1.0
    for dim, parts in pieces:
        draws = jax.random.uniform(jax.random.fold_in(jax.random.fold_in(key, 6), dim), (parts,), jnp.float32, smallest / len(pieces), largest / len(pieces))
        factor_of = factor_of * jnp.repeat(jnp.exp(draws), dims[dim] // parts).reshape((-1,) + (1,) * (len(dims) - 1 - dim))
    return factor_of


def noise(key, dims, width, bound, cuts=(), kind=jnp.bfloat16):
    array = jax.random.normal(key, dims, jnp.float32) * width
    if len(cuts) > 0:
        array = block_levels(key, dims, cuts, -0.22, 0.18) * array
    return jnp.clip(array, min=-bound, max=bound).astype(kind)


def setup_inputs(seed: int = 0) -> dict:
    streams_of = jax.random.split(jax.random.key(seed), 16)
    return {
        "sampled_earlier_tokens": plant(jax.random.randint(streams_of[0], (IMAGES, PREVTOK), 0, VOCAB), jax.random.fold_in(streams_of[0], 1), 0, VOCAB - 1).astype(jnp.int32),
        "quantizer_vectors": noise(streams_of[1], (VOCAB, CVAE), 1.0, 6.0, (), jnp.float32),
        "summed_latent_canvas": noise(streams_of[2], (IMAGES, TOK, CVAE), 1.0, 6.0, ((0, 8),), jnp.float32),
        "latent_lift_matrix": noise(streams_of[3], (CVAE, D), CVAE ** -0.5, 1.0, (), jnp.float32),
        "location_tier_offset": noise(streams_of[4], (TOK, D), 0.5, 3.0, (), jnp.float32),
        "adaptive_norm_factors": noise(streams_of[5], (LAYERS, IMAGES, 6, D), 0.5, 3.0, ((1, 8),), jnp.float32),
        "logit_sharpness": draw_logit_sharpness(jax.random.fold_in(streams_of[15], 71), 0),
        "probe_match_content_matrix": draw_probe_match_content_matrix(jax.random.fold_in(streams_of[15], 71), 0),
        "mixing_projection_matrix": noise(streams_of[8], (LAYERS, D, D), D ** -0.5, 0.15625, ((1, 4), (2, 8))),
        "widening_projection_matrix": noise(streams_of[9], (LAYERS, D, FF), D ** -0.5, 0.15625, ((1, 8), (2, 4))),
        "narrowing_projection_matrix": noise(streams_of[10], (LAYERS, FF, D), FF ** -0.5, 0.078125, ((1, 4), (2, 8))),
        "cached_lower_grid_lookups": noise(streams_of[11], (LAYERS, IMAGES, CACHE, D), 1.0, 6.0, ((1, 8), (3, 4))),
        "cached_lower_grid_payloads": noise(streams_of[12], (LAYERS, IMAGES, CACHE, D), 1.0, 6.0, ((1, 8), (3, 4))),
        "final_norm_factors": noise(streams_of[13], (IMAGES, 2, D), 0.5, 3.0, ((0, 8),), jnp.float32),
        "vocabulary_logit_matrix": noise(streams_of[14], (D, VOCAB), D ** -0.5, 0.15625, ((1, 4),)),
    }


norm_floor = 0.1
highest = lax.Precision.HIGHEST

def interp_matrix(grid_side, prev_side):
    out_cells = jnp.arange(grid_side, dtype=jnp.int32)
    numerator = jnp.maximum((2 * out_cells + 1) * prev_side - grid_side, 0)
    lower_cell = numerator // (2 * grid_side)
    fraction = (numerator % (2 * grid_side)).astype(jnp.float32) / (2.0 * grid_side)
    upper_cell = jnp.minimum(lower_cell + 1, prev_side - 1)
    in_cells = jnp.arange(prev_side, dtype=jnp.int32)
    lower_hit = (in_cells[None, :] == lower_cell[:, None]).astype(jnp.float32)
    upper_hit = (in_cells[None, :] == upper_cell[:, None]).astype(jnp.float32)
    return lower_hit * (1.0 - fraction)[:, None] + upper_hit * fraction[:, None]

def modulate(stream, scale_vec, shift_vec):
    center = stream - lax.optimization_barrier(jnp.mean(stream, axis=-1, keepdims=True))
    variance = lax.optimization_barrier(jnp.mean(center * center, axis=-1, keepdims=True))
    return center * lax.rsqrt(variance + norm_floor) * (1.0 + scale_vec) + shift_vec

def hidden_neuron_slice(vectors):
    return vectors * lax.rsqrt(lax.optimization_barrier(jnp.sum(vectors * vectors, axis=-1, keepdims=True)) + 1.0)

def group_sum(left_rows, weight, groups):
    part_width = left_rows.shape[1] // groups
    running = jnp.zeros((left_rows.shape[0], weight.shape[1]), jnp.float32)
    for group_id in range(groups):
        partial_value = jnp.dot(left_rows[:, group_id * part_width:(group_id + 1) * part_width], weight[group_id * part_width:(group_id + 1) * part_width], preferred_element_type=jnp.float32)
        rounded = lax.optimization_barrier(partial_value.astype(jnp.bfloat16))
        running = running + rounded.astype(jnp.float32)
    return running

def attend_image(operands):
    probe_token_slab, keys_all, values_all = operands
    scores = jnp.einsum('thd,shd->hts', probe_token_slab.astype(jnp.float32), keys_all.astype(jnp.float32), precision=highest)
    row_max = lax.optimization_barrier(jnp.max(scores, axis=-1, keepdims=True))
    shifted = jnp.exp(scores - row_max)
    weights_bf = (shifted / lax.optimization_barrier(jnp.sum(shifted, axis=-1, keepdims=True))).astype(jnp.bfloat16)
    attended = jnp.einsum('hts,shd->thd', weights_bf.astype(jnp.float32), values_all.astype(jnp.float32), precision=highest)
    return attended.astype(jnp.bfloat16)

def reference(sampled_earlier_tokens, quantizer_vectors, summed_latent_canvas, latent_lift_matrix, location_tier_offset, adaptive_norm_factors, logit_sharpness, probe_match_content_matrix, mixing_projection_matrix, widening_projection_matrix, narrowing_projection_matrix, cached_lower_grid_lookups, cached_lower_grid_payloads, final_norm_factors, vocabulary_logit_matrix):
    vocab_ids = jnp.arange(VOCAB, dtype=jnp.int32)

    def embed_image(token_ids):
        onehot = (token_ids[:, None] == vocab_ids[None, :]).astype(jnp.float32)
        return jnp.dot(onehot, quantizer_vectors, precision=highest, preferred_element_type=jnp.float32)
    embedded = lax.map(embed_image, sampled_earlier_tokens).reshape(IMAGES, PREV, PREV, CVAE)
    up_matrix = interp_matrix(SIDE, PREV)
    lifted = jnp.einsum('ai,nijc->najc', up_matrix, embedded, precision=highest)
    lifted = jnp.einsum('bj,najc->nabc', up_matrix, lifted, precision=highest)
    canvas = summed_latent_canvas + lifted.reshape(IMAGES, TOK, CVAE)
    stream = jnp.einsum('ntc,cd->ntd', canvas, latent_lift_matrix, precision=highest) + location_tier_offset[None]
    for depth_ordinal in range(LAYERS):
        factors = adaptive_norm_factors[depth_ordinal]
        normed = modulate(stream, factors[:, 2][:, None], factors[:, 4][:, None]).astype(jnp.bfloat16)
        projected = jnp.dot(normed.reshape(IMAGES * TOK, D), probe_match_content_matrix[depth_ordinal].reshape(D, 3 * D), preferred_element_type=jnp.float32)
        complete_channel_group_set = projected.reshape(IMAGES, TOK, 3, HEADS, HDIM)
        probe_token_slab = (hidden_neuron_slice(complete_channel_group_set[:, :, 0]) * logit_sharpness[depth_ordinal][None, None, :, None]).astype(jnp.bfloat16)
        key_new = hidden_neuron_slice(complete_channel_group_set[:, :, 1]).astype(jnp.bfloat16)
        value_new = complete_channel_group_set[:, :, 2].astype(jnp.bfloat16)
        key_old = hidden_neuron_slice(cached_lower_grid_lookups[depth_ordinal].astype(jnp.float32).reshape(IMAGES, CACHE, HEADS, HDIM)).astype(jnp.bfloat16)
        value_old = cached_lower_grid_payloads[depth_ordinal].reshape(IMAGES, CACHE, HEADS, HDIM)
        keys_all = jnp.concatenate([key_old, key_new], axis=1)
        values_all = jnp.concatenate([value_old, value_new], axis=1)
        attended = lax.map(attend_image, (probe_token_slab, keys_all, values_all))
        mixed_rows = group_sum(attended.reshape(IMAGES * TOK, D), mixing_projection_matrix[depth_ordinal], N_TENSOR)
        stream = stream + factors[:, 0][:, None] * mixed_rows.reshape(IMAGES, TOK, D)
        normed = modulate(stream, factors[:, 3][:, None], factors[:, 5][:, None]).astype(jnp.bfloat16)
        hidden = jax.nn.gelu(jnp.dot(normed.reshape(IMAGES * TOK, D), widening_projection_matrix[depth_ordinal], preferred_element_type=jnp.float32), approximate=True).astype(jnp.bfloat16)
        mixed_rows = group_sum(hidden, narrowing_projection_matrix[depth_ordinal], N_TENSOR)
        stream = stream + factors[:, 1][:, None] * mixed_rows.reshape(IMAGES, TOK, D)
    normed = modulate(stream, final_norm_factors[:, 0][:, None], final_norm_factors[:, 1][:, None]).astype(jnp.bfloat16)
    logits = jnp.dot(normed.reshape(IMAGES * TOK, D), vocabulary_logit_matrix, preferred_element_type=jnp.float32).astype(jnp.bfloat16)
    return (logits.reshape(IMAGES, TOK, VOCAB), canvas)
```

```python
import functools
from types import SimpleNamespace
from typing import Any, NamedTuple

import jax
import jax.numpy as jnp
import numpy as np
from jax import lax
from jax.experimental import pallas as pl
from jax.experimental.pallas import tpu as pltpu
from jax.sharding import PartitionSpec as P

SIDE = 16
PREV = 13
MESH = pl.DeviceIdType.MESH
norm_floor = 0.1
highest = lax.Precision.HIGHEST
bf16 = jnp.bfloat16
f32 = jnp.float32


def interp_matrix(grid_side, prev_side):
    out_cells = np.arange(grid_side)
    numerator = np.maximum((2 * out_cells + 1) * prev_side - grid_side, 0)
    lower_cell = numerator // (2 * grid_side)
    fraction = (numerator % (2 * grid_side)) / (2.0 * grid_side)
    upper_cell = np.minimum(lower_cell + 1, prev_side - 1)
    in_cells = np.arange(prev_side)
    lower_hit = (in_cells[None, :] == lower_cell[:, None]).astype(np.float64)
    upper_hit = (in_cells[None, :] == upper_cell[:, None]).astype(np.float64)
    return lower_hit * (1.0 - fraction)[:, None] + upper_hit * fraction[:, None]


def modulate(stream, scale_vec, shift_vec):
    center = stream - jnp.mean(stream, axis=-1, keepdims=True)
    variance = jnp.mean(center * center, axis=-1, keepdims=True)
    return center * lax.rsqrt(variance + norm_floor) * (1.0 + scale_vec) + shift_vec


def unit(vectors):
    return vectors * lax.rsqrt(jnp.sum(vectors * vectors, axis=-1, keepdims=True) + 1.0)


def dot(left, right):
    return jnp.dot(left, right, preferred_element_type=f32)


def dot_t(left, right):
    return lax.dot_general(left, right, (((1,), (1,)), ((), ())), preferred_element_type=f32)


def loop(total, body, scope=None):
    def step(index, carry):
        if scope is None:
            body(index)
        else:
            with jax.named_scope(scope):
                body(index)
        return carry

    lax.fori_loop(0, total, step, 0)


QKV, OUT, UP, DOWN = range(4)
EARLY = ((UP, 0), (DOWN, 0))


class Relay:
    def __init__(self, outer, shard_rows, buffers, parts, early, sems):
        self.outer, self.rows, self.buffers, self.parts = outer, shard_rows, buffers, parts
        self.early = early
        self.dp, self.t = lax.axis_index("dp"), lax.axis_index("tensor")
        self.o, self.p = self.dp // 2, lax.rem(self.dp, 2)
        self.z_recv, self.up_send, self.down_send, self.y_recv, self.y_send = sems
        self.number = {}
        for matrix, count in enumerate(parts):
            for part in range(count):
                self.number[(matrix, part)] = len(self.number)

    def ref(self, chunk, o, plane):
        matrix, part = chunk
        count = self.parts[matrix]
        rows = self.rows // count
        p = self.p if plane == 0 else 1 - self.p
        if matrix == DOWN:
            part = part + p * (count - 1 - 2 * part)
        if matrix == QKV:
            start = (o * 2 + p) * self.rows
            rows = self.rows
            return self.buffers[matrix].at[part, pl.ds(pl.multiple_of(start, rows), rows)]
        start = (o * 2 + p) * self.rows + part * rows
        return self.buffers[matrix].at[pl.ds(pl.multiple_of(start, rows), rows)]

    def copy(self, way, chunk, src, plane):
        ref = self.ref(chunk, src, plane)
        number = self.number[chunk]
        if way == "y":
            target = self.o * 2 + 1 - self.p
            send, recv = self.y_send.at[number, src], self.y_recv.at[number, src]
        else:
            target = self.dp + 2 if way == "up" else self.dp - 2
            sends = self.up_send if way == "up" else self.down_send
            send, recv = sends.at[number, plane, src], self.z_recv.at[number, plane, src]
        return pltpu.make_async_remote_copy(
            src_ref=ref, dst_ref=ref, send_sem=send, recv_sem=recv,
            device_id=(target, self.t), device_id_type=MESH,
        )

    def sends(self, way, chunk, src, plane, act):
        room = {"up": self.o < self.outer - 1, "down": self.o > 0, "y": None}[way]
        if room is None:
            act(self.copy(way, chunk, src, plane))
        else:
            pl.when(room)(lambda: act(self.copy(way, chunk, src, plane)))

    def crosses_early(self, chunk):
        return chunk in self.early

    def start_y(self, chunk, act=lambda copy: copy.start()):
        self.sends("y", chunk, self.o, 0, act)

    def start_z(self, chunk, plane=0, act=lambda copy: copy.start()):
        for way in ("up", "down"):
            self.sends(way, chunk, self.o, plane, act)

    def own_z(self, chunks):
        for chunk in chunks:
            self.start_z(chunk)

    def own_y(self, chunks):
        for chunk in chunks:
            if not self.crosses_early(chunk):
                self.start_y(chunk)

    def cross_z(self, chunks):
        for chunk in chunks:
            if self.crosses_early(chunk):
                self.wait_y(chunk, self.o)
                self.start_z(chunk, 1)

    def cross_rest(self, chunks):
        def rest(src):
            @pl.when(src != self.o)
            def _():
                for chunk in chunks:
                    self.sends("y", chunk, src, 0, lambda copy: copy.start())

        loop(self.outer, rest)

    def wait_y(self, chunk, src):
        ref = self.ref(chunk, src, 1)
        number = self.number[chunk]
        pltpu.make_async_remote_copy(
            src_ref=ref, dst_ref=ref, send_sem=self.y_send.at[number, src],
            recv_sem=self.y_recv.at[number, src],
            device_id=(self.o * 2 + 1 - self.p, self.t), device_id_type=MESH,
        ).wait_recv()

    def wait_y_all(self, chunks):
        with jax.named_scope("wait_y"):
            self.wait_y_each(chunks)

    def wait_y_each(self, chunks):
        for chunk in chunks:
            if not self.crosses_early(chunk):
                loop(self.outer, lambda src: self.wait_y(chunk, src))

    def step(self, chunks, s):
        with jax.named_scope("relay"):
            self.step_inner(chunks, s)

    def step_inner(self, chunks, s):
        for chunk in chunks:
            early = self.crosses_early(chunk)
            for plane in (0, 1) if early else (0,):
                for way, src, there in (
                    ("up", self.o - s, self.o >= s),
                    ("down", self.o + s, self.o + s < self.outer),
                ):

                    @pl.when(there)
                    def _():
                        ref = self.ref(chunk, src, plane)
                        number = self.number[chunk]
                        pltpu.make_async_remote_copy(
                            src_ref=ref, dst_ref=ref,
                            send_sem=self.up_send.at[number, plane, src],
                            recv_sem=self.z_recv.at[number, plane, src],
                            device_id=(self.o * 2 + 1 - self.p, self.t), device_id_type=MESH,
                        ).wait_recv()
                        self.sends(way, chunk, src, plane, lambda copy: copy.start())
                        if not early and chunk[0] != OUT:
                            self.sends("y", chunk, src, plane, lambda copy: copy.start())

    def steps(self, chunks, third):
        span = self.outer - 1
        low, high = 1 + third * span // 3, 1 + (third + 1) * span // 3
        if high - low == 1:
            self.step(chunks, low)
        elif high > low:
            loop(high - low, lambda index: self.step(chunks, low + index))

    def drain(self):
        def done(copy):
            copy.wait_send()

        for chunk in self.number:
            early = self.crosses_early(chunk)
            for plane in (0, 1) if early else (0,):

                def sent(src):
                    @pl.when(src <= self.o)
                    def _():
                        self.sends("up", chunk, src, plane, done)

                    @pl.when(src >= self.o)
                    def _():
                        self.sends("down", chunk, src, plane, done)

                    if not early:
                        self.sends("y", chunk, src, plane, done)

                loop(self.outer, sent)
            if early:
                self.start_y(chunk, done)


class Given(NamedTuple):
    ids: Any
    codes: Any
    summed: Any
    lift: Any
    offset: Any
    factors: Any
    sharp: Any
    qkv: Any
    out: Any
    up: Any
    down: Any
    keys: Any
    values: Any
    head_factors: Any
    vocab: Any
    grow: Any


INPUTS = Given._fields


def scratch_shapes(dims):
    outer, rows, images, tokens = dims.outer, dims.rows, dims.images, dims.tokens
    width, heads_width, units = dims.width, dims.heads_width, dims.units
    prev, channels, vocab, codes = dims.prev, dims.channels, dims.vocab, dims.codes
    cache, half, blocks = dims.cache, dims.half, dims.blocks
    chunks = sum(dims.parts)
    dma = pltpu.SemaphoreType.DMA
    block = width // blocks
    return dict(
        w_qkv=pltpu.VMEM((3, width, heads_width), bf16),
        w_out=pltpu.VMEM((width, heads_width), bf16),
        w_up=pltpu.VMEM((width, units), bf16),
        w_down=pltpu.VMEM((width, units), bf16),
        s_ids=pltpu.VMEM((images, prev), jnp.int32),
        s_codes=pltpu.VMEM((channels, codes), f32),
        code_parts=pltpu.VMEM((3 * channels, codes), bf16),
        s_summed=pltpu.VMEM((images, channels, tokens), f32),
        canvas_v=pltpu.VMEM((images, channels, tokens), f32),
        s_lift=pltpu.VMEM((channels, width), f32),
        s_offset=pltpu.VMEM((tokens, width), f32),
        s_factors=pltpu.VMEM((6, images, width), f32),
        s_head_factors=pltpu.VMEM((images, 2, width), f32),
        s_keys=pltpu.VMEM((images, cache, heads_width), bf16),
        s_values=pltpu.VMEM((images, cache, heads_width), bf16),
        all_keys=pltpu.VMEM((images, dims.heads, tokens + cache, heads_width // dims.heads), bf16),
        all_values=pltpu.VMEM((images, dims.heads, tokens + cache, 128), bf16),
        s_vocab=pltpu.VMEM((width, vocab), bf16),
        s_grow=pltpu.VMEM((tokens, prev), f32),
        normed=pltpu.VMEM((images, tokens, width), bf16),
        normed2=pltpu.VMEM((images, tokens, width), bf16),
        normed3=pltpu.VMEM((images, tokens, width), bf16),
        gain=pltpu.VMEM((half, 1, width), f32),
        stream=pltpu.VMEM((half, tokens, width), f32),
        projected=pltpu.VMEM((tokens, 3 * heads_width), f32),
        attended=pltpu.VMEM((images, tokens, heads_width), bf16),
        hidden=pltpu.VMEM((images, tokens, units), bf16),
        near_out0=pltpu.VMEM((half, tokens, width), bf16),
        near_in0=pltpu.VMEM((half, tokens, width), bf16),
        far_out0=pltpu.VMEM((half, tokens, width), bf16),
        far_in0=pltpu.VMEM((half, tokens, width), bf16),
        near_out1=pltpu.VMEM((blocks, half, tokens, block), bf16),
        near_in1=pltpu.VMEM((blocks, half, tokens, block), bf16),
        far_out1=pltpu.VMEM((blocks, half, tokens, block), bf16),
        far_in1=pltpu.VMEM((blocks, half, tokens, block), bf16),
        logits_v=pltpu.VMEM((images, tokens, vocab), bf16),
        z_recv=dma((chunks, 2, outer)),
        up_send=dma((chunks, 2, outer)),
        down_send=dma((chunks, 2, outer)),
        y_recv=dma((chunks, outer)),
        y_send=dma((chunks, outer)),
        load=dma((len(INPUTS),)),
        store=dma((images + 1,)),
        near0=dma((2, half)),
        far0=dma((2, half)),
        near1=dma((2, blocks, 3, half)),
        far1=dma((2, blocks, 3, half)),
        swap2=dma((2, half)),
        swap3=dma((2, half)),
    )


class Bag:
    def __init__(self, names, values):
        self.__dict__.update(zip(names, values))


def step_kernel(dims, *refs):
    outer, rows, images, tokens = dims.outer, dims.rows, dims.images, dims.tokens
    width, heads_width, units = dims.width, dims.heads_width, dims.units
    head_total, head_size = dims.heads, dims.heads_width // dims.heads
    half, blocks, vocab = dims.half, dims.blocks, dims.vocab
    block = width // blocks
    given = Given(*refs[: len(INPUTS)])
    logits_hbm, canvas_hbm = refs[len(INPUTS) : len(INPUTS) + 2]
    v = Bag(list(scratch_shapes(dims)), refs[len(INPUTS) + 2 :])

    relay = Relay(
        outer, rows, (v.w_qkv, v.w_out, v.w_up, v.w_down), dims.parts, dims.early,
        (v.z_recv, v.up_send, v.down_send, v.y_recv, v.y_send),
    )
    dp, t, o, p = relay.dp, relay.t, relay.o, relay.p
    core = lax.rem(t, 2)
    near_t = t + 1 - 2 * core
    far_t = lax.rem(t + 2, 4)
    own_rows = pl.ds(pl.multiple_of(dp * rows, rows), rows)

    loads = {}

    spot = Given(*range(len(INPUTS)))

    def load(index, target):
        loads[index] = pltpu.make_async_copy(given[index], target, v.load.at[index])
        loads[index].start()

    load(spot.qkv, v.w_qkv.at[:, own_rows])
    load(spot.out, v.w_out.at[own_rows])
    load(spot.up, v.w_up.at[own_rows])
    load(spot.codes, v.s_codes)
    load(spot.ids, v.s_ids)
    load(spot.grow, v.s_grow)
    load(spot.summed, v.s_summed)
    load(spot.lift, v.s_lift)
    load(spot.offset, v.s_offset)
    load(spot.factors, v.s_factors)
    load(spot.down, v.w_down.at[own_rows])
    load(spot.keys, v.s_keys)
    load(spot.values, v.s_values)
    load(spot.head_factors, v.s_head_factors)
    load(spot.vocab, v.s_vocab)

    barrier = pltpu.get_barrier_semaphore()

    def greet(target):
        pl.semaphore_signal(barrier, inc=1, device_id=target, device_id_type=MESH)

    greet((o * 2 + 1 - p, t))
    greet((dp, near_t))
    greet((dp, far_t))
    pl.when(o > 0)(lambda: greet((dp - 2, t)))
    pl.when(o < outer - 1)(lambda: greet((dp + 2, t)))
    ends = jnp.where(o > 0, 1, 0) + jnp.where(o < outer - 1, 1, 0)
    pl.semaphore_wait(barrier, 3 + ends)

    chunks = [
        [(matrix, part) for part in range(count)] for matrix, count in enumerate(dims.parts)
    ]
    first = chunks[QKV] + chunks[OUT]

    def begin_y(group):
        for chunk in group:
            if relay.crosses_early(chunk):
                relay.start_y(chunk)

    loads[spot.qkv].wait()
    begin_y(chunks[QKV])
    relay.own_z(chunks[QKV])
    relay.own_y(chunks[QKV])
    loads[spot.out].wait()
    begin_y(chunks[OUT])
    relay.own_z(chunks[OUT])

    loads[spot.codes].wait()
    channels = dims.channels

    def split_codes(tile):
        cols = pl.ds(pl.multiple_of(tile * 512, 512), 512)
        left = v.s_codes[:, cols]
        for part in range(3):
            piece = left.astype(bf16)
            v.code_parts[part * channels : (part + 1) * channels, cols] = piece
            left = left - piece.astype(f32)

    with jax.named_scope("split_codes"):
        loop(dims.codes // 512, split_codes)
    for name in (spot.ids, spot.grow, spot.summed, spot.lift, spot.offset, spot.factors):
        loads[name].wait()

    inner = jnp.logical_and(o > 0, o < outer - 1)

    def inside(when, act):
        pl.when(jnp.logical_and(inner, when))(act)

    def at_end(when, act):
        pl.when(jnp.logical_and(jnp.logical_not(inner), when))(act)

    def image_of(slot):
        return lax.rem(half * (1 - core) + slot, images)

    prev = dims.prev
    vocab_tile = 1024

    def factor(row, image, cols=slice(None)):
        return v.s_factors[row, pl.ds(image, 1), cols]

    def embed(slot):
        image = image_of(slot)
        ids_row = v.s_ids[pl.ds(image, 1), :].astype(f32)
        same = lax.broadcasted_iota(jnp.int32, (prev, prev), 0) == lax.broadcasted_iota(
            jnp.int32, (prev, prev), 1
        )
        ids = jnp.sum(jnp.where(same, ids_row, 0.0), axis=1, keepdims=True)

        def codes_tile(tile, total):
            place = lax.broadcasted_iota(jnp.int32, (prev, vocab_tile), 1).astype(f32) + (
                tile * vocab_tile
            ).astype(f32)
            onehot = jnp.where(ids == place, 1.0, 0.0).astype(bf16)
            cols = pl.ds(pl.multiple_of(tile * vocab_tile, vocab_tile), vocab_tile)
            return total + dot_t(v.code_parts[:, cols], onehot)

        parts = lax.fori_loop(
            0, dims.codes // vocab_tile, codes_tile, jnp.zeros((3 * channels, prev), f32)
        )
        embedded = parts[:channels] + parts[channels : 2 * channels] + parts[2 * channels :]
        grown = lax.dot_general(
            embedded, v.s_grow[...], (((1,), (1,)), ((), ())), precision=highest,
            preferred_element_type=f32,
        )
        canvas = v.s_summed[image] + grown
        v.canvas_v[image] = canvas
        stream = (
            jnp.dot(canvas.T, v.s_lift[...], precision=highest, preferred_element_type=f32)
            + v.s_offset[...]
        )
        v.normed[slot] = modulate(stream, factor(2, image), factor(4, image)).astype(bf16)

        @pl.when(slot >= half)
        def _():
            v.stream[slot - half] = stream

        for head in range(head_total):
            low = head * head_size
            high = low + head_size
            old = slice(tokens, tokens + dims.cache)
            v.all_keys[image, head, old, :] = unit(
                v.s_keys[image, :, low:high].astype(f32)
            ).astype(bf16)
            v.all_values[image, head] = jnp.ones((tokens + dims.cache, 128), bf16)
            v.all_values[image, head, old, :head_size] = v.s_values[image, :, low:high]

        @pl.when(slot == 1)
        def _():
            relay.cross_z(first)
            relay.steps(first, 0)
            begin_y(chunks[UP])

        @pl.when(slot == 2)
        def _():
            relay.steps(first, 1)
            relay.own_z(chunks[UP])

        @pl.when(slot == 3)
        def _():
            relay.steps(first, 2)
            if not relay.crosses_early((OUT, 0)):
                relay.own_y(chunks[OUT])
                relay.cross_rest(chunks[OUT])
            relay.own_y(chunks[UP])
            begin_y(chunks[DOWN])

    loads[spot.keys].wait()
    loads[spot.values].wait()
    loads[spot.up].wait()
    loads[spot.down].wait()
    loop(images, embed, "embed")
    canvas_out = pltpu.make_async_copy(v.canvas_v, canvas_hbm, v.store.at[images])
    canvas_out.start()
    relay.cross_z(chunks[UP])
    relay.wait_y_all(chunks[QKV])

    def near_copy(name, sems, index):
        source, target = name
        return pltpu.make_async_remote_copy(
            src_ref=source, dst_ref=target, send_sem=sems.at[(0, *index)],
            recv_sem=sems.at[(1, *index)], device_id=(dp, near_t), device_id_type=MESH,
        )

    def far_copy(name, sems, index):
        source, target = name
        return pltpu.make_async_remote_copy(
            src_ref=source, dst_ref=target, send_sem=sems.at[(0, *index)],
            recv_sem=sems.at[(1, *index)], device_id=(dp, far_t), device_id_type=MESH,
        )

    def near0(j):
        return near_copy((v.near_out0.at[j], v.near_in0.at[j]), v.near0, (j,))

    def far0(j):
        return far_copy((v.far_out0.at[j], v.far_in0.at[j]), v.far0, (j,))

    def near1(n, j, piece, turn):
        name = (v.near_out1.at[n, j, :, piece], v.near_in1.at[n, j, :, piece])
        return near_copy(name, v.near1, (n, turn, j))

    def far1(n, j, piece, turn):
        name = (v.far_out1.at[n, j, :, piece], v.far_in1.at[n, j, :, piece])
        return far_copy(name, v.far1, (n, turn, j))

    def swap2(j):
        return near_copy((v.normed2.at[half + j], v.normed2.at[j]), v.swap2, (j,))

    def swap3(j):
        return near_copy((v.normed3.at[half + j], v.normed3.at[j]), v.swap3, (j,))

    def attend(turn):
        slot = slot_of(turn)
        image = image_of(slot)

        @pl.when(turn == 2)
        def _():
            inside(True, lambda: relay.steps(chunks[UP], 1))
            relay.own_z(chunks[DOWN])
            relay.cross_z(chunks[DOWN])
            inside(True, lambda: relay.own_y(chunks[DOWN]))

        def project(tile):
            cols = pl.ds(pl.multiple_of(tile * heads_width, heads_width), heads_width)
            v.projected[:, cols] = dot(v.normed[slot], v.w_qkv[tile])

        loop(3, project)
        for head in range(head_total):
            low = head * head_size
            high = low + head_size
            query = (unit(v.projected[:, low:high]) * given.sharp[0, head]).astype(bf16)
            key_new = unit(v.projected[:, heads_width + low : heads_width + high]).astype(bf16)
            value_new = v.projected[:, 2 * heads_width + low : 2 * heads_width + high].astype(bf16)
            keys, values = v.all_keys.at[image, head], v.all_values.at[image, head]
            keys[:tokens, :] = key_new
            values[:tokens, :head_size] = value_new
            scores = dot_t(query, keys[...])
            weights = jnp.exp(scores - jnp.max(scores, axis=-1, keepdims=True)).astype(bf16)
            mixed = dot(weights, values[...])
            total = mixed[:, head_size : head_size + 1]
            v.attended[slot, :, low:high] = (mixed[:, :head_size] / total).astype(bf16)
            if head == 1:
                at_end(turn == 1, lambda: relay.steps(chunks[UP], 0))
                at_end(turn == 3, lambda: relay.steps(chunks[UP], 1))

        inside(turn == 0, lambda: relay.steps(chunks[UP], 0))

        @pl.when(turn == 1)
        def _():
            relay.wait_y_all(chunks[OUT])

        @pl.when(turn > 0)
        def _():
            loop(jnp.where(turn == 1, 2, 1), lambda back: project_out(turn - jnp.where(turn == 1, 1, 0) + back))

    def slot_of(turn):
        return turn // 2 + half * lax.rem(turn, 2)

    def project_out(turn):
        slot = slot_of(turn)
        image = image_of(slot)

        @pl.when(slot >= half)
        def _():
            near0(slot - half).wait_recv()

        def out_tile(tile):
            cols = pl.ds(pl.multiple_of(tile * block, block), block)
            partial = dot_t(v.attended[slot], v.w_out[cols, :])

            @pl.when(slot < half)
            def _():
                v.near_out0[slot, :, cols] = partial.astype(bf16)

            @pl.when(slot >= half)
            def _():
                pair = partial + v.near_in0[slot - half, :, cols].astype(f32)
                v.far_out0[slot - half, :, cols] = pair.astype(bf16)
                v.stream[slot - half, :, cols] += factor(0, image, cols) * pair

        loop(blocks, out_tile)
        pl.when(slot < half)(lambda: near0(slot).start())
        pl.when(slot >= half)(lambda: far0(slot - half).start())

    loop(images, attend, "attend")

    def second_norm(j):
        image = image_of(half + j)
        v.gain[j] = factor(1, image)
        far0(j).wait_recv()
        stream = v.stream[j] + factor(0, image) * v.far_in0[j].astype(f32)
        v.stream[j] = stream
        v.normed2[half + j] = modulate(stream, factor(3, image), factor(5, image)).astype(bf16)
        swap2(j).start()

    def second_norms(j):
        second_norm(j)

        @pl.when(j == 0)
        def _():
            relay.steps(chunks[UP], 2)
            at_end(True, lambda: relay.own_y(chunks[DOWN]))
            inside(True, lambda: relay.steps(chunks[DOWN], 0))

    loop(half, second_norms, "second_norm")
    relay.wait_y_all(chunks[UP])

    unit_tile = 512

    def lift_units(turn):
        slot = turn // 2 + half * (1 - lax.rem(turn, 2))
        pl.when(slot < half)(lambda: swap2(slot).wait_recv())

        def tile_units(tile):
            cols = pl.ds(pl.multiple_of(tile * unit_tile, unit_tile), unit_tile)
            lifted = dot(v.normed2[slot], v.w_up[:, cols])
            v.hidden[slot, :, cols] = jax.nn.gelu(lifted, approximate=True).astype(bf16)

        loop(units // unit_tile, tile_units)
        at_end(turn == 1, lambda: relay.steps(chunks[DOWN], 0))
        inside(turn == 1, lambda: relay.steps(chunks[DOWN], 1))

    loop(images, lift_units, "lift_units")

    both = jnp.minimum(o, outer - 1 - o)
    sign = jnp.where(o < outer - 1 - o, 1, -1)

    def block_of(n):
        if blocks != outer:
            return n
        distance = (n + 1) // 2
        beside = o + distance * (1 - 2 * lax.rem(n, 2))
        beyond = o + sign * (n - both)
        return jnp.where(n <= 2 * both, beside, beyond)

    if blocks != outer:
        at_end(True, lambda: relay.steps(chunks[DOWN], 1))
        relay.steps(chunks[DOWN], 2)
        relay.wait_y_all(chunks[DOWN])

    def wait_down(n, parts):
        if blocks == outer:
            for chunk in parts:
                if not relay.crosses_early(chunk):
                    relay.wait_y(chunk, block_of(n))

    def down_piece(n, low, size):
        start = block_of(n) * block + low
        cols = pl.ds(pl.multiple_of(start, 128), size)
        piece = slice(low, low + size)
        turn = low // size

        def theirs(j):
            v.near_out1[n, j, :, piece] = dot_t(v.hidden[j], v.w_down[cols, :]).astype(bf16)
            near1(n, j, piece, turn).start()

        loop(half, theirs)

        def ours(j):
            partial = dot_t(v.hidden[half + j], v.w_down[cols, :])
            near1(n, j, piece, turn).wait_recv()
            pair = partial + v.near_in1[n, j, :, piece].astype(f32)
            v.far_out1[n, j, :, piece] = pair.astype(bf16)
            far1(n, j, piece, turn).start()
            v.stream[j, :, cols] += v.gain[j, :, cols] * pair

        loop(half, ours)

    def add_far(n, j, low, size):
        start = block_of(n) * block + low
        cols = pl.ds(pl.multiple_of(start, 128), size)
        piece = slice(low, low + size)
        far1(n, j, piece, low // size).wait_recv()
        v.stream[j, :, cols] += v.gain[j, :, cols] * v.far_in1[n, j, :, piece].astype(f32)

    def down_block(n):
        if blocks == outer:
            at_end(n == 1, lambda: relay.steps(chunks[DOWN], 1))
            pl.when(n == 2)(lambda: relay.steps(chunks[DOWN], 2))
        with jax.named_scope("wait_down"):
            wait_down(n, chunks[DOWN])
        down_piece(n, 0, block)

        @pl.when(n > 0)
        def _():
            loop(half, lambda j: add_far(n - 1, j, 0, block))

    loop(blocks - 1, down_block, "down_block")
    end = blocks - 1
    part = block // 3
    most = 2 * len(chunks[DOWN]) // 3
    with jax.named_scope("last_wait"):
        wait_down(end, chunks[DOWN][:most])
    down_piece(end, 0, part)
    down_piece(end, 2 * part, part)
    loop(half, lambda j: add_far(end - 1, j, 0, block))
    with jax.named_scope("last_wait"):
        wait_down(end, chunks[DOWN][most:])
    down_piece(end, part, part)
    with jax.named_scope("drain"):
        relay.drain()
    loads[spot.head_factors].wait()
    loads[spot.vocab].wait()

    def last_norm(j):
        image = image_of(half + j)
        for low in (0, 2 * part, part):
            add_far(end, j, low, part)
        factors = v.s_head_factors.at[image]
        v.normed3[half + j] = modulate(
            v.stream[j], factors[0:1, :], factors[1:2, :]
        ).astype(bf16)
        swap3(j).start()

    loop(half, last_norm, "last_norm")

    def logits_out(image):
        return pltpu.make_async_copy(
            v.logits_v.at[image], logits_hbm.at[image], v.store.at[image]
        )

    def give_logits(turn):
        slot = lax.rem(turn + half, images)
        image = image_of(slot)
        pl.when(slot < half)(lambda: swap3(slot).wait_recv())
        v.logits_v[image] = dot(v.normed3[slot], v.s_vocab[...]).astype(bf16)
        logits_out(image).start()

    loop(images, give_logits, "give_logits")

    def finish(j):
        near0(j).wait_send()
        far0(j).wait_send()
        swap2(j).wait_send()
        swap3(j).wait_send()

        def block_done(n):
            near1(n, j, slice(0, block), 0).wait_send()
            far1(n, j, slice(0, block), 0).wait_send()

        loop(blocks - 1, block_done)
        for low in (0, part, 2 * part):
            piece = slice(low, low + part)
            near1(end, j, piece, low // part).wait_send()
            far1(end, j, piece, low // part).wait_send()

    loop(half, finish)
    loop(images, lambda image: logits_out(image).wait())
    canvas_out.wait()


def local(
    dp_total, tensor_total, ids, codes, summed, lift, offset, factors, sharp, qkv, out, up, down,
    keys, values, head_factors, vocab,
):
    images, prev = ids.shape
    tokens, width = offset.shape
    rows = qkv.shape[1]
    outer = dp_total // 2
    group = 1
    while (2 * rows * group) % 128:
        group *= 2
    heads_width = out.shape[1]
    assert tensor_total == 4 and images % 2 == 0 and dp_total % 2 == 0
    down_parts = 6 if rows % 96 == 0 else 3
    dims = SimpleNamespace(
        outer=outer, rows=rows, images=images, tokens=tokens, width=width,
        heads_width=heads_width, heads=sharp.shape[1], units=up.shape[2],
        prev=prev, channels=codes.shape[1], codes=codes.shape[0],
        vocab=vocab.shape[1], cache=keys.shape[2], half=images // 2,
        blocks=outer // group, parts=(3, 1, 3, down_parts), early=EARLY,
    )
    grow = interp_matrix(SIDE, PREV)
    grow = jnp.asarray(np.kron(grow, grow), f32)
    given = (
        ids, codes.T, summed.swapaxes(1, 2), lift, offset, factors[0].swapaxes(0, 1), sharp,
        qkv[0].swapaxes(0, 1), out[0].T, up[0], down[0].T, keys[0], values[0],
        head_factors, vocab, grow,
    )
    anywhere = pl.BlockSpec(memory_space=pl.ANY)
    specs = [anywhere] * len(INPUTS)
    specs[Given(*range(len(INPUTS))).sharp] = pl.BlockSpec(memory_space=pltpu.SMEM)
    logits, canvas = pl.pallas_call(
        functools.partial(step_kernel, dims),
        out_shape=(
            jax.ShapeDtypeStruct((images, tokens, vocab.shape[1]), bf16),
            jax.ShapeDtypeStruct((images, summed.shape[2], tokens), f32),
        ),
        in_specs=specs,
        out_specs=(anywhere, anywhere),
        scratch_shapes=list(scratch_shapes(dims).values()),
        compiler_params=pltpu.CompilerParams(
            collective_id=0, has_side_effects=True, vmem_limit_bytes=67043328
        ),
        name="step",
    )(*given)
    return logits, canvas.swapaxes(1, 2)


def solution(mesh):
    placed = (
        P("dp", None),
        P(),
        P("dp", None, None),
        P(),
        P(),
        P(None, "dp", None, None),
        P(None, "tensor"),
        P(None, "dp", None, "tensor"),
        P(None, "tensor", "dp"),
        P(None, "dp", "tensor"),
        P(None, "tensor", "dp"),
        P(None, "dp", None, "tensor"),
        P(None, "dp", None, "tensor"),
        P("dp", None, None),
        P(None, "tensor"),
    )
    return jax.shard_map(
        functools.partial(local, mesh.shape["dp"], mesh.shape["tensor"]),
        mesh=mesh,
        in_specs=placed,
        out_specs=(P("dp", None, "tensor"), P("dp", None, None)),
        check_vma=False,
    )
```

```python
import functools
from types import SimpleNamespace
from typing import Any, NamedTuple

import jax
import jax.numpy as jnp
import numpy as np
from jax import lax
from jax.experimental import pallas as pl
from jax.experimental.pallas import tpu as pltpu
from jax.sharding import PartitionSpec as P

SIDE = 16
PREV = 13
MESH = pl.DeviceIdType.MESH
norm_floor = 0.1
highest = lax.Precision.HIGHEST
bf16 = jnp.bfloat16
f32 = jnp.float32


def interp_matrix(grid_side, prev_side):
    out_cells = np.arange(grid_side)
    numerator = np.maximum((2 * out_cells + 1) * prev_side - grid_side, 0)
    lower_cell = numerator // (2 * grid_side)
    fraction = (numerator % (2 * grid_side)) / (2.0 * grid_side)
    upper_cell = np.minimum(lower_cell + 1, prev_side - 1)
    in_cells = np.arange(prev_side)
    lower_hit = (in_cells[None, :] == lower_cell[:, None]).astype(np.float64)
    upper_hit = (in_cells[None, :] == upper_cell[:, None]).astype(np.float64)
    return lower_hit * (1.0 - fraction)[:, None] + upper_hit * fraction[:, None]


def modulate(stream, scale_vec, shift_vec):
    center = stream - jnp.mean(stream, axis=-1, keepdims=True)
    variance = jnp.mean(center * center, axis=-1, keepdims=True)
    return center * lax.rsqrt(variance + norm_floor) * (1.0 + scale_vec) + shift_vec


def unit(vectors):
    return vectors * lax.rsqrt(jnp.sum(vectors * vectors, axis=-1, keepdims=True) + 1.0)


def dot(left, right):
    return jnp.dot(left, right, preferred_element_type=f32)


def dot_t(left, right):
    return lax.dot_general(left, right, (((1,), (1,)), ((), ())), preferred_element_type=f32)


def loop(total, body, scope=None):
    def step(index, carry):
        if scope is None:
            body(index)
        else:
            with jax.named_scope(scope):
                body(index)
        return carry

    lax.fori_loop(0, total, step, 0)


QKV, OUT, UP, DOWN = range(4)
EARLY = ((UP, 0), (DOWN, 0))


class Relay:
    def __init__(self, outer, shard_rows, buffers, parts, early, sems):
        self.outer, self.rows, self.buffers, self.parts = outer, shard_rows, buffers, parts
        self.early = early
        self.dp, self.t = lax.axis_index("dp"), lax.axis_index("tensor")
        self.o, self.p = self.dp // 2, lax.rem(self.dp, 2)
        self.z_recv, self.z_send, self.y_recv, self.y_each, self.y_send = sems
        self.number, self.lane = {}, {}
        for matrix, count in enumerate(parts):
            for part in range(count):
                self.number[(matrix, part)] = len(self.number)
        for chunk in self.number:
            self.lane[chunk, 0] = len(self.lane)
        for chunk in early:
            self.lane[chunk, 1] = len(self.lane)

    def span(self, chunk, copies):
        matrix, part = chunk
        if matrix == QKV:
            return self.buffers[matrix].at[part, pl.ds(0, copies * self.rows)]
        return self.buffers[matrix].at[pl.ds(0, copies * (self.rows // self.parts[matrix]))]

    def wait(self, ref, send=None, recv=None):
        copy = pltpu.make_async_remote_copy(
            src_ref=ref, dst_ref=ref,
            send_sem=recv if send is None else send, recv_sem=send if recv is None else recv,
            device_id=(self.o * 2 + 1 - self.p, self.t), device_id_type=MESH,
        )
        if send is None:
            copy.wait_recv()
        else:
            copy.wait_send()

    def ref(self, chunk, o, plane):
        matrix, part = chunk
        count = self.parts[matrix]
        rows = self.rows // count
        p = self.p if plane == 0 else 1 - self.p
        if matrix == DOWN:
            part = part + p * (count - 1 - 2 * part)
        if matrix == QKV:
            start = (o * 2 + p) * self.rows
            rows = self.rows
            return self.buffers[matrix].at[part, pl.ds(pl.multiple_of(start, rows), rows)]
        start = (o * 2 + p) * self.rows + part * rows
        return self.buffers[matrix].at[pl.ds(pl.multiple_of(start, rows), rows)]

    def y_arrival(self, chunk, src):
        if chunk[0] == DOWN and not self.crosses_early(chunk):
            return self.y_each.at[chunk[1], src]
        return self.y_recv.at[self.number[chunk]]

    def copy(self, way, chunk, src, plane):
        ref = self.ref(chunk, src, plane)
        if way == "y":
            target = self.o * 2 + 1 - self.p
            send, recv = self.y_send.at[self.number[chunk]], self.y_arrival(chunk, src)
        else:
            lane = self.lane[chunk, plane]
            target = self.dp + 2 if way == "up" else self.dp - 2
            send = self.z_send.at[lane]
            recv = self.z_recv.at[lane, src if way == "up" else src - 1]
        return pltpu.make_async_remote_copy(
            src_ref=ref, dst_ref=ref, send_sem=send, recv_sem=recv,
            device_id=(target, self.t), device_id_type=MESH,
        )

    def sends(self, way, chunk, src, plane, act):
        room = {"up": self.o < self.outer - 1, "down": self.o > 0, "y": None}[way]
        if room is None:
            act(self.copy(way, chunk, src, plane))
        else:
            pl.when(room)(lambda: act(self.copy(way, chunk, src, plane)))

    def crosses_early(self, chunk):
        return chunk in self.early

    def start_y(self, chunk, act=lambda copy: copy.start()):
        self.sends("y", chunk, self.o, 0, act)

    def start_z(self, chunk, plane=0, act=lambda copy: copy.start()):
        for way in ("up", "down"):
            self.sends(way, chunk, self.o, plane, act)

    def own_z(self, chunks):
        for chunk in chunks:
            self.start_z(chunk)

    def own_y(self, chunks):
        for chunk in chunks:
            if not self.crosses_early(chunk):
                self.start_y(chunk)

    def cross_z(self, chunks):
        for chunk in chunks:
            if self.crosses_early(chunk):
                self.wait_y(chunk, self.o)
                self.start_z(chunk, 1)

    def cross_rest(self, chunks):
        def rest(src):
            @pl.when(src != self.o)
            def _():
                for chunk in chunks:
                    self.sends("y", chunk, src, 0, lambda copy: copy.start())

        loop(self.outer, rest)

    def wait_y(self, chunk, src):
        self.wait(self.ref(chunk, src, 1), recv=self.y_arrival(chunk, src))

    def wait_y_all(self, chunks):
        with jax.named_scope("wait_y"):
            for chunk in chunks:
                if self.crosses_early(chunk):
                    continue
                if chunk[0] == DOWN:
                    loop(self.outer, lambda src: self.wait_y(chunk, src))
                else:
                    self.wait(self.span(chunk, self.outer), recv=self.y_arrival(chunk, 0))

    def step(self, chunks, s):
        below = ("up", self.o - s, self.o >= s)
        above = ("down", self.o + s, self.o + s < self.outer)
        with jax.named_scope("relay"):
            if chunks[0][0] == DOWN:
                for side in (below, above):
                    for chunk in chunks:
                        self.pass_on(chunk, *side)
            else:
                for chunk in chunks:
                    for side in (below, above):
                        self.pass_on(chunk, *side)

    def pass_on(self, chunk, way, src, there):
        early = self.crosses_early(chunk)

        @pl.when(there)
        def _():
            for plane in (0, 1) if early else (0,):
                arrived = self.z_recv.at[self.lane[chunk, plane], src if way == "up" else src - 1]
                self.wait(self.ref(chunk, src, plane), recv=arrived)
                self.sends(way, chunk, src, plane, lambda copy: copy.start())
                if not early and chunk[0] != OUT:
                    self.sends("y", chunk, src, plane, lambda copy: copy.start())

    def steps(self, chunks, third):
        span = self.outer - 1
        low, high = 1 + third * span // 3, 1 + (third + 1) * span // 3
        if high - low == 1:
            self.step(chunks, low)
        elif high > low:
            loop(high - low, lambda index: self.step(chunks, low + index))

    def drain(self):
        inner = jnp.logical_and(self.o > 0, self.o < self.outer - 1)
        for (chunk, plane), lane in self.lane.items():
            sent = self.z_send.at[lane]

            @pl.when(inner)
            def _():
                self.wait(self.span(chunk, self.outer + 1), send=sent)

            @pl.when(jnp.logical_not(inner))
            def _():
                self.wait(self.span(chunk, 1), send=sent)

        for chunk, number in self.number.items():
            copies = 1 if self.crosses_early(chunk) else self.outer
            self.wait(self.span(chunk, copies), send=self.y_send.at[number])


class Given(NamedTuple):
    ids: Any
    codes: Any
    summed: Any
    lift: Any
    offset: Any
    factors: Any
    sharp: Any
    qkv: Any
    out: Any
    up: Any
    down: Any
    keys: Any
    values: Any
    head_factors: Any
    vocab: Any
    grow: Any


INPUTS = Given._fields


def scratch_shapes(dims):
    outer, rows, images, tokens = dims.outer, dims.rows, dims.images, dims.tokens
    width, heads_width, units = dims.width, dims.heads_width, dims.units
    prev, channels, vocab, codes = dims.prev, dims.channels, dims.vocab, dims.codes
    cache, half, blocks = dims.cache, dims.half, dims.blocks
    chunks = sum(dims.parts)
    lanes = chunks + len(dims.early)
    dma = pltpu.SemaphoreType.DMA
    block = width // blocks
    return dict(
        w_qkv=pltpu.VMEM((3, width, heads_width), bf16),
        w_out=pltpu.VMEM((width, heads_width), bf16),
        w_up=pltpu.VMEM((width, units), bf16),
        w_down=pltpu.VMEM((width, units), bf16),
        s_ids=pltpu.VMEM((images, prev), jnp.int32),
        s_codes=pltpu.VMEM((channels, codes), f32),
        code_parts=pltpu.VMEM((3 * channels, codes), bf16),
        s_summed=pltpu.VMEM((images, channels, tokens), f32),
        canvas_v=pltpu.VMEM((images, channels, tokens), f32),
        s_lift=pltpu.VMEM((channels, width), f32),
        s_offset=pltpu.VMEM((tokens, width), f32),
        s_factors=pltpu.VMEM((6, images, width), f32),
        s_head_factors=pltpu.VMEM((images, 2, width), f32),
        s_keys=pltpu.VMEM((images, cache, heads_width), bf16),
        s_values=pltpu.VMEM((images, cache, heads_width), bf16),
        all_keys=pltpu.VMEM((images, dims.heads, tokens + cache, heads_width // dims.heads), bf16),
        all_values=pltpu.VMEM((images, dims.heads, tokens + cache, 128), bf16),
        s_vocab=pltpu.VMEM((width, vocab), bf16),
        s_grow=pltpu.VMEM((tokens, prev), f32),
        normed=pltpu.VMEM((images, tokens, width), bf16),
        normed2=pltpu.VMEM((images, tokens, width), bf16),
        normed3=pltpu.VMEM((images, tokens, width), bf16),
        gain=pltpu.VMEM((half, 1, width), f32),
        stream=pltpu.VMEM((half, tokens, width), f32),
        projected=pltpu.VMEM((tokens, 3 * heads_width), f32),
        attended=pltpu.VMEM((images, tokens, heads_width), bf16),
        hidden=pltpu.VMEM((images, tokens, units), bf16),
        near_out0=pltpu.VMEM((half, tokens, width), bf16),
        near_in0=pltpu.VMEM((half, tokens, width), bf16),
        far_out0=pltpu.VMEM((half, tokens, width), bf16),
        far_in0=pltpu.VMEM((half, tokens, width), bf16),
        near_out1=pltpu.VMEM((blocks, half, tokens, block), bf16),
        near_in1=pltpu.VMEM((blocks, half, tokens, block), bf16),
        far_out1=pltpu.VMEM((blocks, half, tokens, block), bf16),
        far_in1=pltpu.VMEM((blocks, half, tokens, block), bf16),
        logits_v=pltpu.VMEM((images, tokens, vocab), bf16),
        z_recv=dma((lanes, outer - 1)),
        z_send=dma((lanes,)),
        y_recv=dma((chunks,)),
        y_each=dma((dims.parts[DOWN], outer)),
        y_send=dma((chunks,)),
        load=dma((len(INPUTS),)),
        store=dma((images + 1,)),
        sent=dma((6,)),
        near0=dma((half,)),
        far0=dma((half,)),
        near1=dma((blocks + 2, half)),
        far1=dma((blocks + 2, half)),
        swap2=dma((half,)),
        swap3=dma((half,)),
    )


class Bag:
    def __init__(self, names, values):
        self.__dict__.update(zip(names, values))


def step_kernel(dims, *refs):
    outer, rows, images, tokens = dims.outer, dims.rows, dims.images, dims.tokens
    width, heads_width, units = dims.width, dims.heads_width, dims.units
    head_total, head_size = dims.heads, dims.heads_width // dims.heads
    half, blocks, vocab = dims.half, dims.blocks, dims.vocab
    block = width // blocks
    given = Given(*refs[: len(INPUTS)])
    logits_hbm, canvas_hbm = refs[len(INPUTS) : len(INPUTS) + 2]
    v = Bag(list(scratch_shapes(dims)), refs[len(INPUTS) + 2 :])

    relay = Relay(
        outer, rows, (v.w_qkv, v.w_out, v.w_up, v.w_down), dims.parts, dims.early,
        (v.z_recv, v.z_send, v.y_recv, v.y_each, v.y_send),
    )
    dp, t, o, p = relay.dp, relay.t, relay.o, relay.p
    core = lax.rem(t, 2)
    near_t = t + 1 - 2 * core
    far_t = lax.rem(t + 2, 4)
    own_rows = pl.ds(pl.multiple_of(dp * rows, rows), rows)

    loads = {}

    spot = Given(*range(len(INPUTS)))

    def load(index, target):
        loads[index] = pltpu.make_async_copy(given[index], target, v.load.at[index])
        loads[index].start()

    load(spot.qkv, v.w_qkv.at[:, own_rows])
    load(spot.out, v.w_out.at[own_rows])
    load(spot.up, v.w_up.at[own_rows])
    load(spot.codes, v.s_codes)
    load(spot.ids, v.s_ids)
    load(spot.grow, v.s_grow)
    load(spot.summed, v.s_summed)
    load(spot.lift, v.s_lift)
    load(spot.offset, v.s_offset)
    load(spot.factors, v.s_factors)
    load(spot.down, v.w_down.at[own_rows])
    load(spot.keys, v.s_keys)
    load(spot.values, v.s_values)
    load(spot.head_factors, v.s_head_factors)
    load(spot.vocab, v.s_vocab)

    barrier = pltpu.get_barrier_semaphore()

    def greet(target):
        pl.semaphore_signal(barrier, inc=1, device_id=target, device_id_type=MESH)

    greet((o * 2 + 1 - p, t))
    greet((dp, near_t))
    greet((dp, far_t))
    pl.when(o > 0)(lambda: greet((dp - 2, t)))
    pl.when(o < outer - 1)(lambda: greet((dp + 2, t)))
    ends = jnp.where(o > 0, 1, 0) + jnp.where(o < outer - 1, 1, 0)
    pl.semaphore_wait(barrier, 3 + ends)

    chunks = [
        [(matrix, part) for part in range(count)] for matrix, count in enumerate(dims.parts)
    ]
    first = chunks[QKV] + chunks[OUT]

    def begin_y(group):
        for chunk in group:
            if relay.crosses_early(chunk):
                relay.start_y(chunk)

    loads[spot.qkv].wait()
    begin_y(chunks[QKV])
    relay.own_z(chunks[QKV])
    relay.own_y(chunks[QKV])
    loads[spot.out].wait()
    begin_y(chunks[OUT])
    relay.own_z(chunks[OUT])

    loads[spot.codes].wait()
    channels = dims.channels

    def split_codes(tile):
        cols = pl.ds(pl.multiple_of(tile * 512, 512), 512)
        left = v.s_codes[:, cols]
        for part in range(3):
            piece = left.astype(bf16)
            v.code_parts[part * channels : (part + 1) * channels, cols] = piece
            left = left - piece.astype(f32)

    with jax.named_scope("split_codes"):
        loop(dims.codes // 512, split_codes)
    for name in (spot.ids, spot.grow, spot.summed, spot.lift, spot.offset, spot.factors):
        loads[name].wait()

    inner = jnp.logical_and(o > 0, o < outer - 1)

    def inside(when, act):
        pl.when(jnp.logical_and(inner, when))(act)

    def at_end(when, act):
        pl.when(jnp.logical_and(jnp.logical_not(inner), when))(act)

    def image_of(slot):
        return lax.rem(half * (1 - core) + slot, images)

    prev = dims.prev
    vocab_tile = 1024

    def factor(row, image, cols=slice(None)):
        return v.s_factors[row, pl.ds(image, 1), cols]

    def embed(slot):
        image = image_of(slot)
        ids_row = v.s_ids[pl.ds(image, 1), :].astype(f32)
        same = lax.broadcasted_iota(jnp.int32, (prev, prev), 0) == lax.broadcasted_iota(
            jnp.int32, (prev, prev), 1
        )
        ids = jnp.sum(jnp.where(same, ids_row, 0.0), axis=1, keepdims=True)

        def codes_tile(tile, total):
            place = lax.broadcasted_iota(jnp.int32, (prev, vocab_tile), 1).astype(f32) + (
                tile * vocab_tile
            ).astype(f32)
            onehot = jnp.where(ids == place, 1.0, 0.0).astype(bf16)
            cols = pl.ds(pl.multiple_of(tile * vocab_tile, vocab_tile), vocab_tile)
            return total + dot_t(v.code_parts[:, cols], onehot)

        parts = lax.fori_loop(
            0, dims.codes // vocab_tile, codes_tile, jnp.zeros((3 * channels, prev), f32)
        )
        embedded = parts[:channels] + parts[channels : 2 * channels] + parts[2 * channels :]
        grown = lax.dot_general(
            embedded, v.s_grow[...], (((1,), (1,)), ((), ())), precision=highest,
            preferred_element_type=f32,
        )
        canvas = v.s_summed[image] + grown
        v.canvas_v[image] = canvas
        stream = (
            jnp.dot(canvas.T, v.s_lift[...], precision=highest, preferred_element_type=f32)
            + v.s_offset[...]
        )
        v.normed[slot] = modulate(stream, factor(2, image), factor(4, image)).astype(bf16)

        @pl.when(slot >= half)
        def _():
            v.stream[slot - half] = stream

        for head in range(head_total):
            low = head * head_size
            high = low + head_size
            old = slice(tokens, tokens + dims.cache)
            v.all_keys[image, head, old, :] = unit(
                v.s_keys[image, :, low:high].astype(f32)
            ).astype(bf16)
            v.all_values[image, head] = jnp.ones((tokens + dims.cache, 128), bf16)
            v.all_values[image, head, old, :head_size] = v.s_values[image, :, low:high]

        @pl.when(slot == 1)
        def _():
            relay.cross_z(first)
            relay.steps(first, 0)
            begin_y(chunks[UP])

        @pl.when(slot == 2)
        def _():
            relay.steps(first, 1)
            relay.own_z(chunks[UP])

        @pl.when(slot == 3)
        def _():
            relay.steps(first, 2)
            if not relay.crosses_early((OUT, 0)):
                relay.own_y(chunks[OUT])
                relay.cross_rest(chunks[OUT])
            relay.own_y(chunks[UP])
            begin_y(chunks[DOWN])

    loads[spot.keys].wait()
    loads[spot.values].wait()
    loads[spot.up].wait()
    loads[spot.down].wait()
    loop(images, embed, "embed")
    canvas_out = pltpu.make_async_copy(v.canvas_v, canvas_hbm, v.store.at[images])
    canvas_out.start()
    relay.cross_z(chunks[UP])
    relay.wait_y_all(chunks[QKV])

    def pair_copy(source, target, lane, recv, t_other):
        return pltpu.make_async_remote_copy(
            src_ref=source, dst_ref=target, send_sem=v.sent.at[lane], recv_sem=recv,
            device_id=(dp, t_other), device_id_type=MESH,
        )

    def near0(j):
        return pair_copy(v.near_out0.at[j], v.near_in0.at[j], 0, v.near0.at[j], near_t)

    def far0(j):
        return pair_copy(v.far_out0.at[j], v.far_in0.at[j], 1, v.far0.at[j], far_t)

    def near1(n, j, piece, turn):
        source, target = v.near_out1.at[n, j, :, piece], v.near_in1.at[n, j, :, piece]
        return pair_copy(source, target, 2, v.near1.at[n + turn, j], near_t)

    def far1(n, j, piece, turn):
        source, target = v.far_out1.at[n, j, :, piece], v.far_in1.at[n, j, :, piece]
        return pair_copy(source, target, 3, v.far1.at[n + turn, j], far_t)

    def swap2(j):
        return pair_copy(v.normed2.at[half + j], v.normed2.at[j], 4, v.swap2.at[j], near_t)

    def swap3(j):
        return pair_copy(v.normed3.at[half + j], v.normed3.at[j], 5, v.swap3.at[j], near_t)

    def attend(turn):
        slot = slot_of(turn)
        image = image_of(slot)

        @pl.when(turn == 2)
        def _():
            inside(True, lambda: relay.steps(chunks[UP], 1))
            relay.own_z(chunks[DOWN])
            relay.cross_z(chunks[DOWN])
            inside(True, lambda: relay.own_y(chunks[DOWN]))

        def project(tile):
            cols = pl.ds(pl.multiple_of(tile * heads_width, heads_width), heads_width)
            v.projected[:, cols] = dot(v.normed[slot], v.w_qkv[tile])

        loop(3, project)
        for head in range(head_total):
            low = head * head_size
            high = low + head_size
            query = (unit(v.projected[:, low:high]) * given.sharp[0, head]).astype(bf16)
            key_new = unit(v.projected[:, heads_width + low : heads_width + high]).astype(bf16)
            value_new = v.projected[:, 2 * heads_width + low : 2 * heads_width + high].astype(bf16)
            keys, values = v.all_keys.at[image, head], v.all_values.at[image, head]
            keys[:tokens, :] = key_new
            values[:tokens, :head_size] = value_new
            scores = dot_t(query, keys[...])
            weights = jnp.exp(scores - jnp.max(scores, axis=-1, keepdims=True)).astype(bf16)
            mixed = dot(weights, values[...])
            total = mixed[:, head_size : head_size + 1]
            v.attended[slot, :, low:high] = (mixed[:, :head_size] / total).astype(bf16)
            if head == 1:
                at_end(turn == 1, lambda: relay.steps(chunks[UP], 0))
                at_end(turn == 3, lambda: relay.steps(chunks[UP], 1))

        inside(turn == 0, lambda: relay.steps(chunks[UP], 0))

        @pl.when(turn == 1)
        def _():
            relay.wait_y_all(chunks[OUT])

        @pl.when(turn > 0)
        def _():
            loop(jnp.where(turn == 1, 2, 1), lambda back: project_out(turn - jnp.where(turn == 1, 1, 0) + back))

    def slot_of(turn):
        return turn // 2 + half * lax.rem(turn, 2)

    def project_out(turn):
        slot = slot_of(turn)
        image = image_of(slot)

        @pl.when(slot >= half)
        def _():
            near0(slot - half).wait_recv()

        def out_tile(tile):
            cols = pl.ds(pl.multiple_of(tile * block, block), block)
            partial = dot_t(v.attended[slot], v.w_out[cols, :])

            @pl.when(slot < half)
            def _():
                v.near_out0[slot, :, cols] = partial.astype(bf16)

            @pl.when(slot >= half)
            def _():
                pair = partial + v.near_in0[slot - half, :, cols].astype(f32)
                v.far_out0[slot - half, :, cols] = pair.astype(bf16)
                v.stream[slot - half, :, cols] += factor(0, image, cols) * pair

        loop(blocks, out_tile)
        pl.when(slot < half)(lambda: near0(slot).start())
        pl.when(slot >= half)(lambda: far0(slot - half).start())

    loop(images, attend, "attend")

    def second_norm(j):
        image = image_of(half + j)
        v.gain[j] = factor(1, image)
        far0(j).wait_recv()
        stream = v.stream[j] + factor(0, image) * v.far_in0[j].astype(f32)
        v.stream[j] = stream
        v.normed2[half + j] = modulate(stream, factor(3, image), factor(5, image)).astype(bf16)
        swap2(j).start()

    def second_norms(j):
        second_norm(j)

        @pl.when(j == 0)
        def _():
            relay.steps(chunks[UP], 2)
            at_end(True, lambda: relay.own_y(chunks[DOWN]))
            inside(True, lambda: relay.steps(chunks[DOWN], 0))

    loop(half, second_norms, "second_norm")
    relay.wait_y_all(chunks[UP])

    unit_tile = 512

    def lift_units(turn):
        slot = turn // 2 + half * (1 - lax.rem(turn, 2))
        pl.when(slot < half)(lambda: swap2(slot).wait_recv())

        def tile_units(tile):
            cols = pl.ds(pl.multiple_of(tile * unit_tile, unit_tile), unit_tile)
            lifted = dot(v.normed2[slot], v.w_up[:, cols])
            v.hidden[slot, :, cols] = jax.nn.gelu(lifted, approximate=True).astype(bf16)

        loop(units // unit_tile, tile_units)
        at_end(turn == 1, lambda: relay.steps(chunks[DOWN], 0))
        inside(turn == 1, lambda: relay.steps(chunks[DOWN], 1))

    loop(images, lift_units, "lift_units")

    both = jnp.minimum(o, outer - 1 - o)
    sign = jnp.where(o < outer - 1 - o, 1, -1)

    def block_of(n):
        if blocks != outer:
            return n
        distance = (n + 1) // 2
        beside = o + distance * (1 - 2 * lax.rem(n, 2))
        beyond = o + sign * (n - both)
        return jnp.where(n <= 2 * both, beside, beyond)

    if blocks != outer:
        at_end(True, lambda: relay.steps(chunks[DOWN], 1))
        relay.steps(chunks[DOWN], 2)
        relay.wait_y_all(chunks[DOWN])

    def wait_down(n, parts):
        if blocks == outer:
            for chunk in parts:
                if not relay.crosses_early(chunk):
                    relay.wait_y(chunk, block_of(n))

    def down_piece(n, low, size):
        start = block_of(n) * block + low
        cols = pl.ds(pl.multiple_of(start, 128), size)
        piece = slice(low, low + size)
        turn = low // size

        def theirs(j):
            v.near_out1[n, j, :, piece] = dot_t(v.hidden[j], v.w_down[cols, :]).astype(bf16)
            near1(n, j, piece, turn).start()

        loop(half, theirs)

        def ours(j):
            partial = dot_t(v.hidden[half + j], v.w_down[cols, :])
            near1(n, j, piece, turn).wait_recv()
            pair = partial + v.near_in1[n, j, :, piece].astype(f32)
            v.far_out1[n, j, :, piece] = pair.astype(bf16)
            far1(n, j, piece, turn).start()
            v.stream[j, :, cols] += v.gain[j, :, cols] * pair

        loop(half, ours)

    def add_far(n, j, low, size):
        start = block_of(n) * block + low
        cols = pl.ds(pl.multiple_of(start, 128), size)
        piece = slice(low, low + size)
        far1(n, j, piece, low // size).wait_recv()
        v.stream[j, :, cols] += v.gain[j, :, cols] * v.far_in1[n, j, :, piece].astype(f32)

    most = 2 * len(chunks[DOWN]) // 3
    front, back = chunks[DOWN][:most], chunks[DOWN][most:]
    end = blocks - 1
    part = block // 3

    def down_relays(n, group):
        if blocks == outer:
            at_end(n == 1, lambda: relay.steps(group, 1))
            pl.when(n == 2)(lambda: relay.steps(group, 2))

    def down_block(n):
        down_relays(n, front)
        with jax.named_scope("wait_down"):
            wait_down(n, chunks[DOWN])
        down_piece(n, 0, block)
        down_relays(n, back)

        @pl.when(n > 1)
        def _():
            loop(half, lambda j: add_far(n - 2, j, 0, block))

    loop(end, down_block, "down_block")
    with jax.named_scope("last_wait"):
        wait_down(end, front)
    down_piece(end, 0, part)
    down_piece(end, 2 * part, part)
    with jax.named_scope("last_wait"):
        wait_down(end, back)
    down_piece(end, part, part)
    loop(half, lambda j: add_far(end - 2, j, 0, block))
    loop(half, lambda j: add_far(end - 1, j, 0, block))
    with jax.named_scope("drain"):
        relay.drain()
    loads[spot.head_factors].wait()
    loads[spot.vocab].wait()

    def last_norm(j):
        image = image_of(half + j)
        for low in (0, 2 * part, part):
            add_far(end, j, low, part)
        factors = v.s_head_factors.at[image]
        v.normed3[half + j] = modulate(
            v.stream[j], factors[0:1, :], factors[1:2, :]
        ).astype(bf16)
        swap3(j).start()

    loop(half, last_norm, "last_norm")

    def logits_out(image):
        return pltpu.make_async_copy(
            v.logits_v.at[image], logits_hbm.at[image], v.store.at[image]
        )

    def give_logits(turn):
        slot = lax.rem(turn + half, images)
        image = image_of(slot)
        pl.when(slot < half)(lambda: swap3(slot).wait_recv())
        v.logits_v[image] = dot(v.normed3[slot], v.s_vocab[...]).astype(bf16)
        logits_out(image).start()

    loop(images, give_logits, "give_logits")

    for lane, source in enumerate(
        (
            v.near_out0, v.far_out0, v.near_out1, v.far_out1,
            v.normed2.at[pl.ds(half, half)], v.normed3.at[pl.ds(half, half)],
        )
    ):
        relay.wait(source, send=v.sent.at[lane])
    loop(images, lambda image: logits_out(image).wait())
    canvas_out.wait()


def local(
    dp_total, tensor_total, ids, codes, summed, lift, offset, factors, sharp, qkv, out, up, down,
    keys, values, head_factors, vocab,
):
    images, prev = ids.shape
    tokens, width = offset.shape
    rows = qkv.shape[1]
    outer = dp_total // 2
    group = 1
    while (2 * rows * group) % 128:
        group *= 2
    heads_width = out.shape[1]
    assert tensor_total == 4 and images % 2 == 0 and dp_total % 2 == 0
    down_parts = 6 if rows % 96 == 0 else 3
    dims = SimpleNamespace(
        outer=outer, rows=rows, images=images, tokens=tokens, width=width,
        heads_width=heads_width, heads=sharp.shape[1], units=up.shape[2],
        prev=prev, channels=codes.shape[1], codes=codes.shape[0],
        vocab=vocab.shape[1], cache=keys.shape[2], half=images // 2,
        blocks=outer // group, parts=(3, 1, 3, down_parts), early=EARLY,
    )
    grow = interp_matrix(SIDE, PREV)
    grow = jnp.asarray(np.kron(grow, grow), f32)
    given = (
        ids, codes.T, summed.swapaxes(1, 2), lift, offset, factors[0].swapaxes(0, 1), sharp,
        qkv[0].swapaxes(0, 1), out[0].T, up[0], down[0].T, keys[0], values[0],
        head_factors, vocab, grow,
    )
    anywhere = pl.BlockSpec(memory_space=pl.ANY)
    specs = [anywhere] * len(INPUTS)
    specs[Given(*range(len(INPUTS))).sharp] = pl.BlockSpec(memory_space=pltpu.SMEM)
    logits, canvas = pl.pallas_call(
        functools.partial(step_kernel, dims),
        out_shape=(
            jax.ShapeDtypeStruct((images, tokens, vocab.shape[1]), bf16),
            jax.ShapeDtypeStruct((images, summed.shape[2], tokens), f32),
        ),
        in_specs=specs,
        out_specs=(anywhere, anywhere),
        scratch_shapes=list(scratch_shapes(dims).values()),
        compiler_params=pltpu.CompilerParams(
            collective_id=0, has_side_effects=True, vmem_limit_bytes=67043328
        ),
        name="step",
    )(*given)
    return logits, canvas.swapaxes(1, 2)


def solution(mesh):
    placed = (
        P("dp", None),
        P(),
        P("dp", None, None),
        P(),
        P(),
        P(None, "dp", None, None),
        P(None, "tensor"),
        P(None, "dp", None, "tensor"),
        P(None, "tensor", "dp"),
        P(None, "dp", "tensor"),
        P(None, "tensor", "dp"),
        P(None, "dp", None, "tensor"),
        P(None, "dp", None, "tensor"),
        P("dp", None, None),
        P(None, "tensor"),
    )
    return jax.shard_map(
        functools.partial(local, mesh.shape["dp"], mesh.shape["tensor"]),
        mesh=mesh,
        in_specs=placed,
        out_specs=(P("dp", None, "tensor"), P("dp", None, None)),
        check_vma=False,
    )
```

```python
import functools
from types import SimpleNamespace
from typing import Any, NamedTuple

import jax
import jax.numpy as jnp
import numpy as np
from jax import lax
from jax.experimental import pallas as pl
from jax.experimental.pallas import tpu as pltpu
from jax.sharding import PartitionSpec as P

SIDE = 16
PREV = 13
MESH = pl.DeviceIdType.MESH
norm_floor = 0.1
highest = lax.Precision.HIGHEST
bf16 = jnp.bfloat16
f32 = jnp.float32


def interp_matrix(grid_side, prev_side):
    out_cells = np.arange(grid_side)
    numerator = np.maximum((2 * out_cells + 1) * prev_side - grid_side, 0)
    lower_cell = numerator // (2 * grid_side)
    fraction = (numerator % (2 * grid_side)) / (2.0 * grid_side)
    upper_cell = np.minimum(lower_cell + 1, prev_side - 1)
    in_cells = np.arange(prev_side)
    lower_hit = (in_cells[None, :] == lower_cell[:, None]).astype(np.float64)
    upper_hit = (in_cells[None, :] == upper_cell[:, None]).astype(np.float64)
    return lower_hit * (1.0 - fraction)[:, None] + upper_hit * fraction[:, None]


def modulate(stream, scale_vec, shift_vec):
    center = stream - jnp.mean(stream, axis=-1, keepdims=True)
    variance = jnp.mean(center * center, axis=-1, keepdims=True)
    return center * lax.rsqrt(variance + norm_floor) * (1.0 + scale_vec) + shift_vec


def unit(vectors):
    return vectors * lax.rsqrt(jnp.sum(vectors * vectors, axis=-1, keepdims=True) + 1.0)


def dot(left, right):
    return jnp.dot(left, right, preferred_element_type=f32)


def dot_t(left, right):
    return lax.dot_general(left, right, (((1,), (1,)), ((), ())), preferred_element_type=f32)


def loop(total, body, scope=None):
    def step(index, carry):
        if scope is None:
            body(index)
        else:
            with jax.named_scope(scope):
                body(index)
        return carry

    lax.fori_loop(0, total, step, 0)


QKV, OUT, UP, DOWN = range(4)
EARLY = ((UP, 0), (DOWN, 0))


class Relay:
    def __init__(self, outer, shard_rows, buffers, parts, early, sems):
        self.outer, self.rows, self.buffers, self.parts = outer, shard_rows, buffers, parts
        self.early = early
        self.dp, self.t = lax.axis_index("dp"), lax.axis_index("tensor")
        self.o, self.p = self.dp // 2, lax.rem(self.dp, 2)
        self.z_recv, self.z_send, self.y_recv, self.y_each, self.y_send = sems
        self.number, self.lane = {}, {}
        for matrix, count in enumerate(parts):
            for part in range(count):
                self.number[(matrix, part)] = len(self.number)
        for chunk in self.number:
            self.lane[chunk, 0] = len(self.lane)
        for chunk in early:
            self.lane[chunk, 1] = len(self.lane)

    def span(self, chunk, copies):
        matrix, part = chunk
        if matrix == QKV:
            return self.buffers[matrix].at[part, pl.ds(0, copies * self.rows)]
        return self.buffers[matrix].at[pl.ds(0, copies * (self.rows // self.parts[matrix]))]

    def wait(self, ref, send=None, recv=None):
        copy = pltpu.make_async_remote_copy(
            src_ref=ref, dst_ref=ref,
            send_sem=recv if send is None else send, recv_sem=send if recv is None else recv,
            device_id=(self.o * 2 + 1 - self.p, self.t), device_id_type=MESH,
        )
        if send is None:
            copy.wait_recv()
        else:
            copy.wait_send()

    def ref(self, chunk, o, plane):
        matrix, part = chunk
        count = self.parts[matrix]
        rows = self.rows // count
        p = self.p if plane == 0 else 1 - self.p
        if matrix == DOWN:
            part = part + p * (count - 1 - 2 * part)
        if matrix == QKV:
            start = (o * 2 + p) * self.rows
            rows = self.rows
            return self.buffers[matrix].at[part, pl.ds(pl.multiple_of(start, rows), rows)]
        start = (o * 2 + p) * self.rows + part * rows
        return self.buffers[matrix].at[pl.ds(pl.multiple_of(start, rows), rows)]

    def y_arrival(self, chunk, src):
        if chunk[0] == DOWN and not self.crosses_early(chunk):
            return self.y_each.at[chunk[1], src]
        return self.y_recv.at[self.number[chunk]]

    def copy(self, way, chunk, src, plane):
        ref = self.ref(chunk, src, plane)
        if way == "y":
            target = self.o * 2 + 1 - self.p
            send, recv = self.y_send.at[self.number[chunk]], self.y_arrival(chunk, src)
        else:
            lane = self.lane[chunk, plane]
            target = self.dp + 2 if way == "up" else self.dp - 2
            send = self.z_send.at[lane]
            recv = self.z_recv.at[lane, src if way == "up" else src - 1]
        return pltpu.make_async_remote_copy(
            src_ref=ref, dst_ref=ref, send_sem=send, recv_sem=recv,
            device_id=(target, self.t), device_id_type=MESH,
        )

    def sends(self, way, chunk, src, plane, act):
        room = {"up": self.o < self.outer - 1, "down": self.o > 0, "y": None}[way]
        if room is None:
            act(self.copy(way, chunk, src, plane))
        else:
            pl.when(room)(lambda: act(self.copy(way, chunk, src, plane)))

    def crosses_early(self, chunk):
        return chunk in self.early

    def start_y(self, chunk, act=lambda copy: copy.start()):
        self.sends("y", chunk, self.o, 0, act)

    def start_z(self, chunk, plane=0, act=lambda copy: copy.start()):
        for way in ("up", "down"):
            self.sends(way, chunk, self.o, plane, act)

    def own_z(self, chunks):
        for chunk in chunks:
            self.start_z(chunk)

    def own_y(self, chunks):
        for chunk in chunks:
            if not self.crosses_early(chunk):
                self.start_y(chunk)

    def cross_z(self, chunks):
        for chunk in chunks:
            if self.crosses_early(chunk):
                self.wait_y(chunk, self.o)
                self.start_z(chunk, 1)

    def cross_rest(self, chunks):
        def rest(src):
            @pl.when(src != self.o)
            def _():
                for chunk in chunks:
                    self.sends("y", chunk, src, 0, lambda copy: copy.start())

        loop(self.outer, rest)

    def wait_y(self, chunk, src):
        self.wait(self.ref(chunk, src, 1), recv=self.y_arrival(chunk, src))

    def wait_y_all(self, chunks):
        with jax.named_scope("wait_y"):
            for chunk in chunks:
                if self.crosses_early(chunk):
                    continue
                if chunk[0] == DOWN:
                    loop(self.outer, lambda src: self.wait_y(chunk, src))
                else:
                    self.wait(self.span(chunk, self.outer), recv=self.y_arrival(chunk, 0))

    def step(self, chunks, s):
        below = ("up", self.o - s, self.o >= s)
        above = ("down", self.o + s, self.o + s < self.outer)
        with jax.named_scope("relay"):
            if chunks[0][0] == DOWN:
                for side in (below, above):
                    for chunk in chunks:
                        self.pass_on(chunk, *side)
            else:
                for chunk in chunks:
                    for side in (below, above):
                        self.pass_on(chunk, *side)

    def pass_on(self, chunk, way, src, there):
        early = self.crosses_early(chunk)

        @pl.when(there)
        def _():
            for plane in (0, 1) if early else (0,):
                arrived = self.z_recv.at[self.lane[chunk, plane], src if way == "up" else src - 1]
                self.wait(self.ref(chunk, src, plane), recv=arrived)
                self.sends(way, chunk, src, plane, lambda copy: copy.start())
                if not early and chunk[0] != OUT:
                    self.sends("y", chunk, src, plane, lambda copy: copy.start())

    def steps(self, chunks, third):
        span = self.outer - 1
        low, high = 1 + third * span // 3, 1 + (third + 1) * span // 3
        if high - low == 1:
            self.step(chunks, low)
        elif high > low:
            loop(high - low, lambda index: self.step(chunks, low + index))

    def drain(self):
        inner = jnp.logical_and(self.o > 0, self.o < self.outer - 1)
        for (chunk, plane), lane in self.lane.items():
            sent = self.z_send.at[lane]

            @pl.when(inner)
            def _():
                self.wait(self.span(chunk, self.outer + 1), send=sent)

            @pl.when(jnp.logical_not(inner))
            def _():
                self.wait(self.span(chunk, 1), send=sent)

        for chunk, number in self.number.items():
            copies = 1 if self.crosses_early(chunk) else self.outer
            self.wait(self.span(chunk, copies), send=self.y_send.at[number])


class Given(NamedTuple):
    ids: Any
    codes: Any
    summed: Any
    lift: Any
    offset: Any
    factors: Any
    sharp: Any
    qkv: Any
    out: Any
    up: Any
    down: Any
    keys: Any
    values: Any
    head_factors: Any
    vocab: Any
    grow: Any


INPUTS = Given._fields


def scratch_shapes(dims):
    outer, rows, images, tokens = dims.outer, dims.rows, dims.images, dims.tokens
    width, heads_width, units = dims.width, dims.heads_width, dims.units
    prev, channels, vocab, codes = dims.prev, dims.channels, dims.vocab, dims.codes
    cache, half, blocks = dims.cache, dims.half, dims.blocks
    chunks = sum(dims.parts)
    lanes = chunks + len(dims.early)
    dma = pltpu.SemaphoreType.DMA
    block = width // blocks
    return dict(
        w_qkv=pltpu.VMEM((3, width, heads_width), bf16),
        w_out=pltpu.VMEM((width, heads_width), bf16),
        w_up=pltpu.VMEM((width, units), bf16),
        w_down=pltpu.VMEM((width, units), bf16),
        s_ids=pltpu.VMEM((images, prev), jnp.int32),
        s_codes=pltpu.VMEM((channels, codes), f32),
        code_parts=pltpu.VMEM((3 * channels, codes), bf16),
        s_summed=pltpu.VMEM((images, channels, tokens), f32),
        canvas_v=pltpu.VMEM((images, channels, tokens), f32),
        s_lift=pltpu.VMEM((channels, width), f32),
        s_offset=pltpu.VMEM((tokens, width), f32),
        s_factors=pltpu.VMEM((6, images, width), f32),
        s_head_factors=pltpu.VMEM((images, 2, width), f32),
        s_keys=pltpu.VMEM((images, cache, heads_width), bf16),
        s_values=pltpu.VMEM((images, cache, heads_width), bf16),
        all_keys=pltpu.VMEM((images, dims.heads, tokens + cache, heads_width // dims.heads), bf16),
        all_values=pltpu.VMEM((images, dims.heads, tokens + cache, 128), bf16),
        s_vocab=pltpu.VMEM((width, vocab), bf16),
        s_grow=pltpu.VMEM((tokens, prev), f32),
        normed=pltpu.VMEM((images, tokens, width), bf16),
        normed2=pltpu.VMEM((images, tokens, width), bf16),
        normed3=pltpu.VMEM((images, tokens, width), bf16),
        gain=pltpu.VMEM((half, 1, width), f32),
        stream=pltpu.VMEM((half, tokens, width), f32),
        projected=pltpu.VMEM((tokens, 3 * heads_width), f32),
        attended=pltpu.VMEM((images, tokens, heads_width), bf16),
        hidden=pltpu.VMEM((images, tokens, units), bf16),
        near_out0=pltpu.VMEM((half, tokens, width), bf16),
        near_in0=pltpu.VMEM((half, tokens, width), bf16),
        far_out0=pltpu.VMEM((half, tokens, width), bf16),
        far_in0=pltpu.VMEM((half, tokens, width), bf16),
        near_out1=pltpu.VMEM((blocks, half, tokens, block), bf16),
        near_in1=pltpu.VMEM((blocks, half, tokens, block), bf16),
        far_out1=pltpu.VMEM((blocks, half, tokens, block), bf16),
        far_in1=pltpu.VMEM((blocks, half, tokens, block), bf16),
        logits_v=pltpu.VMEM((images, tokens, vocab), bf16),
        z_recv=dma((lanes, outer - 1)),
        z_send=dma((lanes,)),
        y_recv=dma((chunks,)),
        y_each=dma((dims.parts[DOWN], outer)),
        y_send=dma((chunks,)),
        load=dma((len(INPUTS),)),
        store=dma((images + 1,)),
        sent=dma((6,)),
        near0=dma((half,)),
        far0=dma((half,)),
        near1=dma((blocks + 2, half)),
        far1=dma((blocks + 2, half)),
        swap2=dma((half,)),
        swap3=dma((half,)),
    )


class Bag:
    def __init__(self, names, values):
        self.__dict__.update(zip(names, values))


def step_kernel(dims, *refs):
    outer, rows, images, tokens = dims.outer, dims.rows, dims.images, dims.tokens
    width, heads_width, units = dims.width, dims.heads_width, dims.units
    head_total, head_size = dims.heads, dims.heads_width // dims.heads
    half, blocks, vocab = dims.half, dims.blocks, dims.vocab
    block = width // blocks
    given = Given(*refs[: len(INPUTS)])
    logits_hbm, canvas_hbm = refs[len(INPUTS) : len(INPUTS) + 2]
    v = Bag(list(scratch_shapes(dims)), refs[len(INPUTS) + 2 :])

    relay = Relay(
        outer, rows, (v.w_qkv, v.w_out, v.w_up, v.w_down), dims.parts, dims.early,
        (v.z_recv, v.z_send, v.y_recv, v.y_each, v.y_send),
    )
    dp, t, o, p = relay.dp, relay.t, relay.o, relay.p
    core = lax.rem(t, 2)
    near_t = t + 1 - 2 * core
    far_t = lax.rem(t + 2, 4)
    own_rows = pl.ds(pl.multiple_of(dp * rows, rows), rows)

    loads = {}

    spot = Given(*range(len(INPUTS)))

    def load(index, target):
        loads[index] = pltpu.make_async_copy(given[index], target, v.load.at[index])
        loads[index].start()

    load(spot.qkv, v.w_qkv.at[:, own_rows])
    load(spot.out, v.w_out.at[own_rows])
    load(spot.up, v.w_up.at[own_rows])
    load(spot.codes, v.s_codes)
    load(spot.ids, v.s_ids)
    load(spot.grow, v.s_grow)
    load(spot.summed, v.s_summed)
    load(spot.lift, v.s_lift)
    load(spot.offset, v.s_offset)
    load(spot.factors, v.s_factors)
    load(spot.down, v.w_down.at[own_rows])
    load(spot.keys, v.s_keys)
    load(spot.values, v.s_values)
    load(spot.head_factors, v.s_head_factors)
    load(spot.vocab, v.s_vocab)

    barrier = pltpu.get_barrier_semaphore()

    def greet(target):
        pl.semaphore_signal(barrier, inc=1, device_id=target, device_id_type=MESH)

    greet((o * 2 + 1 - p, t))
    greet((dp, near_t))
    greet((dp, far_t))
    pl.when(o > 0)(lambda: greet((dp - 2, t)))
    pl.when(o < outer - 1)(lambda: greet((dp + 2, t)))
    ends = jnp.where(o > 0, 1, 0) + jnp.where(o < outer - 1, 1, 0)
    pl.semaphore_wait(barrier, 3 + ends)

    chunks = [
        [(matrix, part) for part in range(count)] for matrix, count in enumerate(dims.parts)
    ]
    first = chunks[QKV] + chunks[OUT]
    up_late = [chunk for chunk in chunks[UP] if chunk not in dims.early]
    up_early = [chunk for chunk in chunks[UP] if chunk in dims.early]

    def begin_y(group):
        for chunk in group:
            if relay.crosses_early(chunk):
                relay.start_y(chunk)

    loads[spot.qkv].wait()
    begin_y(chunks[QKV])
    relay.own_z(chunks[QKV])
    relay.own_y(chunks[QKV])
    loads[spot.out].wait()
    begin_y(chunks[OUT])
    relay.own_z(chunks[OUT])

    loads[spot.codes].wait()
    channels = dims.channels

    def split_codes(tile):
        cols = pl.ds(pl.multiple_of(tile * 512, 512), 512)
        left = v.s_codes[:, cols]
        for part in range(3):
            piece = left.astype(bf16)
            v.code_parts[part * channels : (part + 1) * channels, cols] = piece
            left = left - piece.astype(f32)

    with jax.named_scope("split_codes"):
        loop(dims.codes // 512, split_codes)
    for name in (spot.ids, spot.grow, spot.summed, spot.lift, spot.offset, spot.factors):
        loads[name].wait()

    inner = jnp.logical_and(o > 0, o < outer - 1)

    def inside(when, act):
        pl.when(jnp.logical_and(inner, when))(act)

    def at_end(when, act):
        pl.when(jnp.logical_and(jnp.logical_not(inner), when))(act)

    def image_of(slot):
        return lax.rem(half * (1 - core) + slot, images)

    prev = dims.prev
    vocab_tile = 1024

    def factor(row, image, cols=slice(None)):
        return v.s_factors[row, pl.ds(image, 1), cols]

    def embed(slot):
        image = image_of(slot)
        ids_row = v.s_ids[pl.ds(image, 1), :].astype(f32)
        same = lax.broadcasted_iota(jnp.int32, (prev, prev), 0) == lax.broadcasted_iota(
            jnp.int32, (prev, prev), 1
        )
        ids = jnp.sum(jnp.where(same, ids_row, 0.0), axis=1, keepdims=True)

        def codes_tile(tile, total):
            place = lax.broadcasted_iota(jnp.int32, (prev, vocab_tile), 1).astype(f32) + (
                tile * vocab_tile
            ).astype(f32)
            onehot = jnp.where(ids == place, 1.0, 0.0).astype(bf16)
            cols = pl.ds(pl.multiple_of(tile * vocab_tile, vocab_tile), vocab_tile)
            return total + dot_t(v.code_parts[:, cols], onehot)

        parts = lax.fori_loop(
            0, dims.codes // vocab_tile, codes_tile, jnp.zeros((3 * channels, prev), f32)
        )
        embedded = parts[:channels] + parts[channels : 2 * channels] + parts[2 * channels :]
        grown = lax.dot_general(
            embedded, v.s_grow[...], (((1,), (1,)), ((), ())), precision=highest,
            preferred_element_type=f32,
        )
        canvas = v.s_summed[image] + grown
        v.canvas_v[image] = canvas
        stream = (
            jnp.dot(canvas.T, v.s_lift[...], precision=highest, preferred_element_type=f32)
            + v.s_offset[...]
        )
        v.normed[slot] = modulate(stream, factor(2, image), factor(4, image)).astype(bf16)

        @pl.when(slot >= half)
        def _():
            v.stream[slot - half] = stream

        for head in range(head_total):
            low = head * head_size
            high = low + head_size
            old = slice(tokens, tokens + dims.cache)
            v.all_keys[image, head, old, :] = unit(
                v.s_keys[image, :, low:high].astype(f32)
            ).astype(bf16)
            v.all_values[image, head] = jnp.ones((tokens + dims.cache, 128), bf16)
            v.all_values[image, head, old, :head_size] = v.s_values[image, :, low:high]

        @pl.when(slot == 1)
        def _():
            relay.cross_z(first)
            relay.steps(first, 0)
            begin_y(chunks[UP])

        @pl.when(slot == 2)
        def _():
            relay.steps(first, 1)
            relay.own_z(up_late + up_early)

        @pl.when(slot == 3)
        def _():
            relay.steps(first, 2)
            if not relay.crosses_early((OUT, 0)):
                relay.own_y(chunks[OUT])
                relay.cross_rest(chunks[OUT])
            relay.own_y(chunks[UP])
            begin_y(chunks[DOWN])

    loads[spot.keys].wait()
    loads[spot.values].wait()
    loads[spot.up].wait()
    loads[spot.down].wait()
    loop(images, embed, "embed")
    canvas_out = pltpu.make_async_copy(v.canvas_v, canvas_hbm, v.store.at[images])
    canvas_out.start()
    relay.cross_z(chunks[UP])
    relay.wait_y_all(chunks[QKV])

    def pair_copy(source, target, lane, recv, t_other):
        return pltpu.make_async_remote_copy(
            src_ref=source, dst_ref=target, send_sem=v.sent.at[lane], recv_sem=recv,
            device_id=(dp, t_other), device_id_type=MESH,
        )

    def near0(j):
        return pair_copy(v.near_out0.at[j], v.near_in0.at[j], 0, v.near0.at[j], near_t)

    def far0(j):
        return pair_copy(v.far_out0.at[j], v.far_in0.at[j], 1, v.far0.at[j], far_t)

    def near1(n, j, piece, turn):
        source, target = v.near_out1.at[n, j, :, piece], v.near_in1.at[n, j, :, piece]
        return pair_copy(source, target, 2, v.near1.at[n + turn, j], near_t)

    def far1(n, j, piece, turn):
        source, target = v.far_out1.at[n, j, :, piece], v.far_in1.at[n, j, :, piece]
        return pair_copy(source, target, 3, v.far1.at[n + turn, j], far_t)

    def swap2(j):
        return pair_copy(v.normed2.at[half + j], v.normed2.at[j], 4, v.swap2.at[j], near_t)

    def swap3(j):
        return pair_copy(v.normed3.at[half + j], v.normed3.at[j], 5, v.swap3.at[j], near_t)

    def attend(turn):
        slot = slot_of(turn)
        image = image_of(slot)

        @pl.when(turn == 2)
        def _():
            inside(True, lambda: relay.steps(up_late, 1))

        def project(tile):
            cols = pl.ds(pl.multiple_of(tile * heads_width, heads_width), heads_width)
            v.projected[:, cols] = dot(v.normed[slot], v.w_qkv[tile])

        loop(3, project)
        for head in range(head_total):
            low = head * head_size
            high = low + head_size
            query = (unit(v.projected[:, low:high]) * given.sharp[0, head]).astype(bf16)
            key_new = unit(v.projected[:, heads_width + low : heads_width + high]).astype(bf16)
            value_new = v.projected[:, 2 * heads_width + low : 2 * heads_width + high].astype(bf16)
            keys, values = v.all_keys.at[image, head], v.all_values.at[image, head]
            keys[:tokens, :] = key_new
            values[:tokens, :head_size] = value_new
            scores = dot_t(query, keys[...])
            weights = jnp.exp(scores - jnp.max(scores, axis=-1, keepdims=True)).astype(bf16)
            mixed = dot(weights, values[...])
            total = mixed[:, head_size : head_size + 1]
            v.attended[slot, :, low:high] = (mixed[:, :head_size] / total).astype(bf16)
            if head == 1:
                at_end(turn == 1, lambda: relay.steps(up_late, 0))

                @pl.when(turn == 1)
                def _():
                    relay.wait_y_all(chunks[OUT])
                    project_out(turn - 1)

        inside(turn == 0, lambda: relay.steps(up_late + up_early, 0))

        pl.when(turn > 0)(lambda: project_out(turn))

        at_end(turn == 1, lambda: relay.steps(up_early, 0))

        @pl.when(turn == 2)
        def _():
            inside(True, lambda: relay.steps(up_early, 1))
            relay.own_z(chunks[DOWN])
            relay.cross_z(chunks[DOWN])
            inside(True, lambda: relay.own_y(chunks[DOWN]))
            at_end(True, lambda: relay.steps(up_late, 1))
            at_end(True, lambda: relay.own_y(chunks[DOWN][:3]))

    def slot_of(turn):
        return turn // 2 + half * lax.rem(turn, 2)

    def project_out(turn):
        slot = slot_of(turn)
        image = image_of(slot)

        @pl.when(slot >= half)
        def _():
            near0(slot - half).wait_recv()

        def out_tile(tile):
            cols = pl.ds(pl.multiple_of(tile * block, block), block)
            partial = dot_t(v.attended[slot], v.w_out[cols, :])

            @pl.when(slot < half)
            def _():
                v.near_out0[slot, :, cols] = partial.astype(bf16)

            @pl.when(slot >= half)
            def _():
                pair = partial + v.near_in0[slot - half, :, cols].astype(f32)
                v.far_out0[slot - half, :, cols] = pair.astype(bf16)
                v.stream[slot - half, :, cols] += factor(0, image, cols) * pair

        loop(blocks, out_tile)
        pl.when(slot < half)(lambda: near0(slot).start())
        pl.when(slot >= half)(lambda: far0(slot - half).start())

    loop(images, attend, "attend")

    def second_norm(j):
        image = image_of(half + j)
        v.gain[j] = factor(1, image)
        far0(j).wait_recv()
        stream = v.stream[j] + factor(0, image) * v.far_in0[j].astype(f32)
        v.stream[j] = stream
        v.normed2[half + j] = modulate(stream, factor(3, image), factor(5, image)).astype(bf16)
        swap2(j).start()

    def second_norms(j):
        second_norm(j)

        @pl.when(j == 0)
        def _():
            at_end(True, lambda: relay.steps(up_early, 1))
            relay.steps(up_late, 2)
            at_end(True, lambda: relay.own_y(chunks[DOWN][3:]))
            inside(True, lambda: relay.steps(chunks[DOWN], 0))
            relay.steps(up_early, 2)

    loop(half, second_norms, "second_norm")
    relay.wait_y_all(chunks[UP])

    both = jnp.minimum(o, outer - 1 - o)
    sign = jnp.where(o < outer - 1 - o, 1, -1)

    def block_of(n):
        if blocks != outer:
            return n
        distance = (n + 1) // 2
        beside = o + distance * (1 - 2 * lax.rem(n, 2))
        beyond = o + sign * (n - both)
        return jnp.where(n <= 2 * both, beside, beyond)

    def wait_down(n, parts):
        if blocks == outer:
            for chunk in parts:
                if not relay.crosses_early(chunk):
                    relay.wait_y(chunk, block_of(n))

    def down_piece(n, low, size, first_j=0, count=half):
        start = block_of(n) * block + low
        cols = pl.ds(pl.multiple_of(start, 128), size)
        piece = slice(low, low + size)
        turn = low // size

        def theirs(j):
            v.near_out1[n, j, :, piece] = dot_t(v.hidden[j], v.w_down[cols, :]).astype(bf16)
            near1(n, j, piece, turn).start()

        loop(count, lambda j: theirs(first_j + j))

        def ours(j):
            partial = dot_t(v.hidden[half + j], v.w_down[cols, :])
            near1(n, j, piece, turn).wait_recv()
            pair = partial + v.near_in1[n, j, :, piece].astype(f32)
            v.far_out1[n, j, :, piece] = pair.astype(bf16)
            far1(n, j, piece, turn).start()
            v.stream[j, :, cols] += v.gain[j, :, cols] * pair

        loop(count, lambda j: ours(first_j + j))

    def add_far(n, j, low, size):
        start = block_of(n) * block + low
        cols = pl.ds(pl.multiple_of(start, 128), size)
        piece = slice(low, low + size)
        far1(n, j, piece, low // size).wait_recv()
        v.stream[j, :, cols] += v.gain[j, :, cols] * v.far_in1[n, j, :, piece].astype(f32)

    unit_tile = 512

    def lift_units(turn):
        slot = turn // 2 + half * (1 - lax.rem(turn, 2))
        pl.when(slot < half)(lambda: swap2(slot).wait_recv())

        def tile_units(tile):
            cols = pl.ds(pl.multiple_of(tile * unit_tile, unit_tile), unit_tile)
            lifted = dot(v.normed2[slot], v.w_up[:, cols])
            v.hidden[slot, :, cols] = jax.nn.gelu(lifted, approximate=True).astype(bf16)

        loop(units // unit_tile, tile_units)
        at_end(turn == 1, lambda: relay.steps(chunks[DOWN], 0))
        inside(turn == 1, lambda: relay.steps(chunks[DOWN], 1))
        if blocks == outer:

            @pl.when(lax.rem(turn, 2) == 1)
            def _():
                pl.when(turn == 1)(lambda: wait_down(0, chunks[DOWN]))
                down_piece(0, 0, block, turn // 2, 1)


    loop(images, lift_units, "lift_units")

    if blocks != outer:
        at_end(True, lambda: relay.steps(chunks[DOWN], 1))
        relay.steps(chunks[DOWN], 2)
        relay.wait_y_all(chunks[DOWN])

    most = 2 * len(chunks[DOWN]) // 3
    front, back = chunks[DOWN][:most], chunks[DOWN][most:]
    end = blocks - 1
    skip = 1 if blocks == outer else 0
    part = block // 3

    def down_relays(n, group):
        if blocks == outer:
            at_end(n == 1, lambda: relay.steps(group, 1))
            pl.when(n == 2)(lambda: relay.steps(group, 2))

    def down_block(n):
        n = n + skip
        down_relays(n, chunks[DOWN][:3])
        with jax.named_scope("wait_down"):
            wait_down(n, chunks[DOWN])
        down_piece(n, 0, block)
        down_relays(n, chunks[DOWN][3:])

        @pl.when(n > 1)
        def _():
            loop(half, lambda j: add_far(n - 2, j, 0, block))

    loop(end - skip, down_block, "down_block")
    with jax.named_scope("last_wait"):
        wait_down(end, front)
    down_piece(end, 0, part)
    down_piece(end, 2 * part, part)
    with jax.named_scope("last_wait"):
        wait_down(end, back)
    down_piece(end, part, part)
    loop(half, lambda j: add_far(end - 2, j, 0, block))
    loop(half, lambda j: add_far(end - 1, j, 0, block))
    with jax.named_scope("drain"):
        relay.drain()
    loads[spot.head_factors].wait()
    loads[spot.vocab].wait()

    def last_norm(j):
        image = image_of(half + j)
        for low in (0, 2 * part, part):
            add_far(end, j, low, part)
        factors = v.s_head_factors.at[image]
        v.normed3[half + j] = modulate(
            v.stream[j], factors[0:1, :], factors[1:2, :]
        ).astype(bf16)
        swap3(j).start()

    loop(half, last_norm, "last_norm")

    def logits_out(image):
        return pltpu.make_async_copy(
            v.logits_v.at[image], logits_hbm.at[image], v.store.at[image]
        )

    def give_logits(turn):
        slot = lax.rem(turn + half, images)
        image = image_of(slot)
        pl.when(slot < half)(lambda: swap3(slot).wait_recv())
        v.logits_v[image] = dot(v.normed3[slot], v.s_vocab[...]).astype(bf16)
        logits_out(image).start()

    loop(images, give_logits, "give_logits")

    for lane, source in enumerate(
        (
            v.near_out0, v.far_out0, v.near_out1, v.far_out1,
            v.normed2.at[pl.ds(half, half)], v.normed3.at[pl.ds(half, half)],
        )
    ):
        relay.wait(source, send=v.sent.at[lane])
    loop(images, lambda image: logits_out(image).wait())
    canvas_out.wait()


def local(
    dp_total, tensor_total, ids, codes, summed, lift, offset, factors, sharp, qkv, out, up, down,
    keys, values, head_factors, vocab,
):
    images, prev = ids.shape
    tokens, width = offset.shape
    rows = qkv.shape[1]
    outer = dp_total // 2
    group = 1
    while (2 * rows * group) % 128:
        group *= 2
    heads_width = out.shape[1]
    assert tensor_total == 4 and images % 2 == 0 and dp_total % 2 == 0
    down_parts = 6 if rows % 96 == 0 else 3
    dims = SimpleNamespace(
        outer=outer, rows=rows, images=images, tokens=tokens, width=width,
        heads_width=heads_width, heads=sharp.shape[1], units=up.shape[2],
        prev=prev, channels=codes.shape[1], codes=codes.shape[0],
        vocab=vocab.shape[1], cache=keys.shape[2], half=images // 2,
        blocks=outer // group, parts=(3, 1, 3, down_parts), early=EARLY,
    )
    grow = interp_matrix(SIDE, PREV)
    grow = jnp.asarray(np.kron(grow, grow), f32)
    given = (
        ids, codes.T, summed.swapaxes(1, 2), lift, offset, factors[0].swapaxes(0, 1), sharp,
        qkv[0].swapaxes(0, 1), out[0].T, up[0], down[0].T, keys[0], values[0],
        head_factors, vocab, grow,
    )
    anywhere = pl.BlockSpec(memory_space=pl.ANY)
    specs = [anywhere] * len(INPUTS)
    specs[Given(*range(len(INPUTS))).sharp] = pl.BlockSpec(memory_space=pltpu.SMEM)
    logits, canvas = pl.pallas_call(
        functools.partial(step_kernel, dims),
        out_shape=(
            jax.ShapeDtypeStruct((images, tokens, vocab.shape[1]), bf16),
            jax.ShapeDtypeStruct((images, summed.shape[2], tokens), f32),
        ),
        in_specs=specs,
        out_specs=(anywhere, anywhere),
        scratch_shapes=list(scratch_shapes(dims).values()),
        compiler_params=pltpu.CompilerParams(
            collective_id=0, has_side_effects=True, vmem_limit_bytes=67043328
        ),
        name="step",
    )(*given)
    return logits, canvas.swapaxes(1, 2)


def solution(mesh):
    placed = (
        P("dp", None),
        P(),
        P("dp", None, None),
        P(),
        P(),
        P(None, "dp", None, None),
        P(None, "tensor"),
        P(None, "dp", None, "tensor"),
        P(None, "tensor", "dp"),
        P(None, "dp", "tensor"),
        P(None, "tensor", "dp"),
        P(None, "dp", None, "tensor"),
        P(None, "dp", None, "tensor"),
        P("dp", None, None),
        P(None, "tensor"),
    )
    return jax.shard_map(
        functools.partial(local, mesh.shape["dp"], mesh.shape["tensor"]),
        mesh=mesh,
        in_specs=placed,
        out_specs=(P("dp", None, "tensor"), P("dp", None, None)),
        check_vma=False,
    )
```

```python
import functools
from types import SimpleNamespace
from typing import Any, NamedTuple

import jax
import jax.numpy as jnp
import numpy as np
from jax import lax
from jax.experimental import pallas as pl
from jax.experimental.pallas import tpu as pltpu
from jax.sharding import PartitionSpec as P

SIDE = 16
PREV = 13
MESH = pl.DeviceIdType.MESH
norm_floor = 0.1
highest = lax.Precision.HIGHEST
bf16 = jnp.bfloat16
f32 = jnp.float32


def interp_matrix(grid_side, prev_side):
    out_cells = np.arange(grid_side)
    numerator = np.maximum((2 * out_cells + 1) * prev_side - grid_side, 0)
    lower_cell = numerator // (2 * grid_side)
    fraction = (numerator % (2 * grid_side)) / (2.0 * grid_side)
    upper_cell = np.minimum(lower_cell + 1, prev_side - 1)
    in_cells = np.arange(prev_side)
    lower_hit = (in_cells[None, :] == lower_cell[:, None]).astype(np.float64)
    upper_hit = (in_cells[None, :] == upper_cell[:, None]).astype(np.float64)
    return lower_hit * (1.0 - fraction)[:, None] + upper_hit * fraction[:, None]


def modulate(stream, scale_vec, shift_vec):
    center = stream - jnp.mean(stream, axis=-1, keepdims=True)
    variance = jnp.mean(center * center, axis=-1, keepdims=True)
    return center * lax.rsqrt(variance + norm_floor) * (1.0 + scale_vec) + shift_vec


def unit(vectors):
    return vectors * lax.rsqrt(jnp.sum(vectors * vectors, axis=-1, keepdims=True) + 1.0)


def dot(left, right):
    return jnp.dot(left, right, preferred_element_type=f32)


def dot_t(left, right):
    return lax.dot_general(left, right, (((1,), (1,)), ((), ())), preferred_element_type=f32)


def loop(total, body, scope=None):
    def step(index, carry):
        if scope is None:
            body(index)
        else:
            with jax.named_scope(scope):
                body(index)
        return carry

    lax.fori_loop(0, total, step, 0)


QKV, OUT, UP, DOWN = range(4)
EARLY = ((UP, 0), (DOWN, 0))


class Relay:
    def __init__(self, outer, shard_rows, buffers, parts, early, sems):
        self.outer, self.rows, self.buffers, self.parts = outer, shard_rows, buffers, parts
        self.early = early
        self.dp, self.t = lax.axis_index("dp"), lax.axis_index("tensor")
        self.o, self.p = self.dp // 2, lax.rem(self.dp, 2)
        self.z_recv, self.z_send, self.y_recv, self.y_each, self.y_send = sems
        self.number, self.lane = {}, {}
        for matrix, count in enumerate(parts):
            for part in range(count):
                self.number[(matrix, part)] = len(self.number)
        for chunk in self.number:
            self.lane[chunk, 0] = len(self.lane)
        for chunk in early:
            self.lane[chunk, 1] = len(self.lane)

    def span(self, chunk, copies):
        matrix, part = chunk
        if matrix == QKV:
            return self.buffers[matrix].at[part, pl.ds(0, copies * self.rows)]
        return self.buffers[matrix].at[pl.ds(0, copies * (self.rows // self.parts[matrix]))]

    def wait(self, ref, send=None, recv=None):
        copy = pltpu.make_async_remote_copy(
            src_ref=ref, dst_ref=ref,
            send_sem=recv if send is None else send, recv_sem=send if recv is None else recv,
            device_id=(self.o * 2 + 1 - self.p, self.t), device_id_type=MESH,
        )
        if send is None:
            copy.wait_recv()
        else:
            copy.wait_send()

    def ref(self, chunk, o, plane):
        matrix, part = chunk
        count = self.parts[matrix]
        rows = self.rows // count
        p = self.p if plane == 0 else 1 - self.p
        if matrix == DOWN:
            part = part + p * (count - 1 - 2 * part)
        if matrix == QKV:
            start = (o * 2 + p) * self.rows
            rows = self.rows
            return self.buffers[matrix].at[part, pl.ds(pl.multiple_of(start, rows), rows)]
        start = (o * 2 + p) * self.rows + part * rows
        return self.buffers[matrix].at[pl.ds(pl.multiple_of(start, rows), rows)]

    def y_arrival(self, chunk, src):
        if chunk[0] == DOWN and not self.crosses_early(chunk):
            return self.y_each.at[chunk[1], src]
        return self.y_recv.at[self.number[chunk]]

    def copy(self, way, chunk, src, plane):
        ref = self.ref(chunk, src, plane)
        if way == "y":
            target = self.o * 2 + 1 - self.p
            send, recv = self.y_send.at[self.number[chunk]], self.y_arrival(chunk, src)
        else:
            lane = self.lane[chunk, plane]
            target = self.dp + 2 if way == "up" else self.dp - 2
            send = self.z_send.at[lane]
            recv = self.z_recv.at[lane, src if way == "up" else src - 1]
        return pltpu.make_async_remote_copy(
            src_ref=ref, dst_ref=ref, send_sem=send, recv_sem=recv,
            device_id=(target, self.t), device_id_type=MESH,
        )

    def sends(self, way, chunk, src, plane, act):
        room = {"up": self.o < self.outer - 1, "down": self.o > 0, "y": None}[way]
        if room is None:
            act(self.copy(way, chunk, src, plane))
        else:
            pl.when(room)(lambda: act(self.copy(way, chunk, src, plane)))

    def crosses_early(self, chunk):
        return chunk in self.early

    def start_y(self, chunk, act=lambda copy: copy.start()):
        self.sends("y", chunk, self.o, 0, act)

    def start_z(self, chunk, plane=0, act=lambda copy: copy.start()):
        for way in ("up", "down"):
            self.sends(way, chunk, self.o, plane, act)

    def own_z(self, chunks):
        for chunk in chunks:
            self.start_z(chunk)

    def own_y(self, chunks):
        for chunk in chunks:
            if not self.crosses_early(chunk):
                self.start_y(chunk)

    def cross_z(self, chunks):
        for chunk in chunks:
            if self.crosses_early(chunk):
                self.wait_y(chunk, self.o)
                self.start_z(chunk, 1)

    def cross_rest(self, chunks):
        def rest(src):
            @pl.when(src != self.o)
            def _():
                for chunk in chunks:
                    self.sends("y", chunk, src, 0, lambda copy: copy.start())

        loop(self.outer, rest)

    def wait_y(self, chunk, src):
        self.wait(self.ref(chunk, src, 1), recv=self.y_arrival(chunk, src))

    def wait_y_all(self, chunks):
        with jax.named_scope("wait_y"):
            for chunk in chunks:
                if self.crosses_early(chunk):
                    continue
                if chunk[0] == DOWN:
                    loop(self.outer, lambda src: self.wait_y(chunk, src))
                else:
                    self.wait(self.span(chunk, self.outer), recv=self.y_arrival(chunk, 0))

    def step(self, chunks, s):
        below = ("up", self.o - s, self.o >= s)
        above = ("down", self.o + s, self.o + s < self.outer)
        with jax.named_scope("relay"):
            if chunks[0][0] == DOWN:
                for side in (below, above):
                    for chunk in chunks:
                        self.pass_on(chunk, *side)
            else:
                for chunk in chunks:
                    for side in (below, above):
                        self.pass_on(chunk, *side)

    def pass_on(self, chunk, way, src, there):
        early = self.crosses_early(chunk)

        @pl.when(there)
        def _():
            for plane in (0, 1) if early else (0,):
                arrived = self.z_recv.at[self.lane[chunk, plane], src if way == "up" else src - 1]
                self.wait(self.ref(chunk, src, plane), recv=arrived)
                self.sends(way, chunk, src, plane, lambda copy: copy.start())
                if not early and chunk[0] != OUT:
                    self.sends("y", chunk, src, plane, lambda copy: copy.start())

    def steps(self, chunks, third):
        span = self.outer - 1
        low, high = 1 + third * span // 3, 1 + (third + 1) * span // 3
        if high - low == 1:
            self.step(chunks, low)
        elif high > low:
            loop(high - low, lambda index: self.step(chunks, low + index))

    def drain(self):
        inner = jnp.logical_and(self.o > 0, self.o < self.outer - 1)
        for (chunk, plane), lane in self.lane.items():
            sent = self.z_send.at[lane]

            @pl.when(inner)
            def _():
                self.wait(self.span(chunk, self.outer + 1), send=sent)

            @pl.when(jnp.logical_not(inner))
            def _():
                self.wait(self.span(chunk, 1), send=sent)

        for chunk, number in self.number.items():
            copies = 1 if self.crosses_early(chunk) else self.outer
            self.wait(self.span(chunk, copies), send=self.y_send.at[number])


class Given(NamedTuple):
    ids: Any
    codes: Any
    summed: Any
    lift: Any
    offset: Any
    factors: Any
    sharp: Any
    qkv: Any
    out: Any
    up: Any
    down: Any
    keys: Any
    values: Any
    head_factors: Any
    vocab: Any
    grow: Any


INPUTS = Given._fields


def scratch_shapes(dims):
    outer, rows, images, tokens = dims.outer, dims.rows, dims.images, dims.tokens
    width, heads_width, units = dims.width, dims.heads_width, dims.units
    prev, channels, vocab, codes = dims.prev, dims.channels, dims.vocab, dims.codes
    cache, half, blocks = dims.cache, dims.half, dims.blocks
    chunks = sum(dims.parts)
    lanes = chunks + len(dims.early)
    dma = pltpu.SemaphoreType.DMA
    block = width // blocks
    return dict(
        w_qkv=pltpu.VMEM((3, width, heads_width), bf16),
        w_out=pltpu.VMEM((width, heads_width), bf16),
        w_up=pltpu.VMEM((width, units), bf16),
        w_down=pltpu.VMEM((width, units), bf16),
        s_ids=pltpu.VMEM((images, prev), jnp.int32),
        s_codes=pltpu.VMEM((channels, codes), f32),
        code_parts=pltpu.VMEM((3 * channels, codes), bf16),
        s_summed=pltpu.VMEM((images, channels, tokens), f32),
        canvas_v=pltpu.VMEM((images, channels, tokens), f32),
        s_lift=pltpu.VMEM((channels, width), f32),
        s_offset=pltpu.VMEM((tokens, width), f32),
        s_factors=pltpu.VMEM((6, images, width), f32),
        s_head_factors=pltpu.VMEM((images, 2, width), f32),
        s_keys=pltpu.VMEM((images, cache, heads_width), bf16),
        s_values=pltpu.VMEM((images, cache, heads_width), bf16),
        all_keys=pltpu.VMEM((images, dims.heads, tokens + cache, heads_width // dims.heads), bf16),
        all_values=pltpu.VMEM((images, dims.heads, tokens + cache, 128), bf16),
        s_vocab=pltpu.VMEM((width, vocab), bf16),
        s_grow=pltpu.VMEM((tokens, prev), f32),
        normed=pltpu.VMEM((images, tokens, width), bf16),
        normed2=pltpu.VMEM((images, tokens, width), bf16),
        normed3=pltpu.VMEM((images, tokens, width), bf16),
        gain=pltpu.VMEM((half, 1, width), f32),
        stream=pltpu.VMEM((half, tokens, width), f32),
        projected=pltpu.VMEM((tokens, 3 * heads_width), f32),
        attended=pltpu.VMEM((images, tokens, heads_width), bf16),
        hidden=pltpu.VMEM((images, tokens, units), bf16),
        near_out0=pltpu.VMEM((half, tokens, width), bf16),
        near_in0=pltpu.VMEM((half, tokens, width), bf16),
        far_out0=pltpu.VMEM((half, tokens, width), bf16),
        far_in0=pltpu.VMEM((half, tokens, width), bf16),
        near_out1=pltpu.VMEM((blocks, half, tokens, block), bf16),
        near_in1=pltpu.VMEM((blocks, half, tokens, block), bf16),
        far_out1=pltpu.VMEM((blocks, half, tokens, block), bf16),
        far_in1=pltpu.VMEM((blocks, half, tokens, block), bf16),
        logits_v=pltpu.VMEM((images, tokens, vocab), bf16),
        z_recv=dma((lanes, outer - 1)),
        z_send=dma((lanes,)),
        y_recv=dma((chunks,)),
        y_each=dma((dims.parts[DOWN], outer)),
        y_send=dma((chunks,)),
        load=dma((len(INPUTS),)),
        store=dma((images + 1,)),
        sent=dma((6,)),
        near0=dma((half,)),
        far0=dma((half,)),
        near1=dma((blocks + 2, half)),
        far1=dma((blocks + 2, half)),
        swap2=dma((half,)),
        swap3=dma((half,)),
    )


class Bag:
    def __init__(self, names, values):
        self.__dict__.update(zip(names, values))


def step_kernel(dims, *refs):
    outer, rows, images, tokens = dims.outer, dims.rows, dims.images, dims.tokens
    width, heads_width, units = dims.width, dims.heads_width, dims.units
    head_total, head_size = dims.heads, dims.heads_width // dims.heads
    half, blocks, vocab = dims.half, dims.blocks, dims.vocab
    block = width // blocks
    given = Given(*refs[: len(INPUTS)])
    logits_hbm, canvas_hbm = refs[len(INPUTS) : len(INPUTS) + 2]
    v = Bag(list(scratch_shapes(dims)), refs[len(INPUTS) + 2 :])

    relay = Relay(
        outer, rows, (v.w_qkv, v.w_out, v.w_up, v.w_down), dims.parts, dims.early,
        (v.z_recv, v.z_send, v.y_recv, v.y_each, v.y_send),
    )
    dp, t, o, p = relay.dp, relay.t, relay.o, relay.p
    core = lax.rem(t, 2)
    near_t = t + 1 - 2 * core
    far_t = lax.rem(t + 2, 4)
    own_rows = pl.ds(pl.multiple_of(dp * rows, rows), rows)

    loads = {}

    spot = Given(*range(len(INPUTS)))

    def load(index, target):
        loads[index] = pltpu.make_async_copy(given[index], target, v.load.at[index])
        loads[index].start()

    load(spot.qkv, v.w_qkv.at[:, own_rows])
    load(spot.out, v.w_out.at[own_rows])
    load(spot.up, v.w_up.at[own_rows])
    load(spot.codes, v.s_codes)
    load(spot.ids, v.s_ids)
    load(spot.grow, v.s_grow)
    load(spot.summed, v.s_summed)
    load(spot.lift, v.s_lift)
    load(spot.offset, v.s_offset)
    load(spot.factors, v.s_factors)
    load(spot.down, v.w_down.at[own_rows])
    load(spot.keys, v.s_keys)
    load(spot.values, v.s_values)
    load(spot.head_factors, v.s_head_factors)
    load(spot.vocab, v.s_vocab)

    barrier = pltpu.get_barrier_semaphore()

    def greet(target):
        pl.semaphore_signal(barrier, inc=1, device_id=target, device_id_type=MESH)

    greet((o * 2 + 1 - p, t))
    greet((dp, near_t))
    greet((dp, far_t))
    pl.when(o > 0)(lambda: greet((dp - 2, t)))
    pl.when(o < outer - 1)(lambda: greet((dp + 2, t)))
    ends = jnp.where(o > 0, 1, 0) + jnp.where(o < outer - 1, 1, 0)
    pl.semaphore_wait(barrier, 3 + ends)

    chunks = [
        [(matrix, part) for part in range(count)] for matrix, count in enumerate(dims.parts)
    ]
    first = chunks[QKV] + chunks[OUT]
    up_late = [chunk for chunk in chunks[UP] if chunk not in dims.early]
    up_early = [chunk for chunk in chunks[UP] if chunk in dims.early]

    def begin_y(group):
        for chunk in group:
            if relay.crosses_early(chunk):
                relay.start_y(chunk)

    loads[spot.qkv].wait()
    begin_y(chunks[QKV])
    relay.own_z(chunks[QKV])
    relay.own_y(chunks[QKV])
    loads[spot.out].wait()
    begin_y(chunks[OUT])
    relay.own_z(chunks[OUT])

    loads[spot.codes].wait()
    channels = dims.channels

    def split_codes(tile):
        cols = pl.ds(pl.multiple_of(tile * 512, 512), 512)
        left = v.s_codes[:, cols]
        for part in range(3):
            piece = left.astype(bf16)
            v.code_parts[part * channels : (part + 1) * channels, cols] = piece
            left = left - piece.astype(f32)

    with jax.named_scope("split_codes"):
        loop(dims.codes // 512, split_codes)
    for name in (spot.ids, spot.grow, spot.summed, spot.lift, spot.offset, spot.factors):
        loads[name].wait()

    inner = jnp.logical_and(o > 0, o < outer - 1)

    def inside(when, act):
        pl.when(jnp.logical_and(inner, when))(act)

    def at_end(when, act):
        pl.when(jnp.logical_and(jnp.logical_not(inner), when))(act)

    def image_of(slot):
        return lax.rem(half * (1 - core) + slot, images)

    prev = dims.prev
    vocab_tile = 1024

    def factor(row, image, cols=slice(None)):
        return v.s_factors[row, pl.ds(image, 1), cols]

    def embed(slot):
        image = image_of(slot)
        ids_row = v.s_ids[pl.ds(image, 1), :].astype(f32)
        same = lax.broadcasted_iota(jnp.int32, (prev, prev), 0) == lax.broadcasted_iota(
            jnp.int32, (prev, prev), 1
        )
        ids = jnp.sum(jnp.where(same, ids_row, 0.0), axis=1, keepdims=True)

        def codes_tile(tile, total):
            place = lax.broadcasted_iota(jnp.int32, (prev, vocab_tile), 1).astype(f32) + (
                tile * vocab_tile
            ).astype(f32)
            onehot = jnp.where(ids == place, 1.0, 0.0).astype(bf16)
            cols = pl.ds(pl.multiple_of(tile * vocab_tile, vocab_tile), vocab_tile)
            return total + dot_t(v.code_parts[:, cols], onehot)

        parts = lax.fori_loop(
            0, dims.codes // vocab_tile, codes_tile, jnp.zeros((3 * channels, prev), f32)
        )
        embedded = parts[:channels] + parts[channels : 2 * channels] + parts[2 * channels :]
        grown = lax.dot_general(
            embedded, v.s_grow[...], (((1,), (1,)), ((), ())), precision=highest,
            preferred_element_type=f32,
        )
        canvas = v.s_summed[image] + grown
        v.canvas_v[image] = canvas
        stream = (
            jnp.dot(canvas.T, v.s_lift[...], precision=highest, preferred_element_type=f32)
            + v.s_offset[...]
        )
        v.normed[slot] = modulate(stream, factor(2, image), factor(4, image)).astype(bf16)

        @pl.when(slot >= half)
        def _():
            v.stream[slot - half] = stream

        for head in range(head_total):
            low = head * head_size
            high = low + head_size
            old = slice(tokens, tokens + dims.cache)
            v.all_keys[image, head, old, :] = unit(
                v.s_keys[image, :, low:high].astype(f32)
            ).astype(bf16)
            v.all_values[image, head] = jnp.ones((tokens + dims.cache, 128), bf16)
            v.all_values[image, head, old, :head_size] = v.s_values[image, :, low:high]

        @pl.when(slot == 1)
        def _():
            relay.cross_z(first)
            relay.steps(first, 0)

        @pl.when(slot == 2)
        def _():
            relay.steps(first, 1)
            relay.own_z(up_late + up_early)

        @pl.when(slot == 3)
        def _():
            relay.steps(first, 2)
            begin_y(chunks[UP])
            if not relay.crosses_early((OUT, 0)):
                relay.own_y(chunks[OUT])
                relay.cross_rest(chunks[OUT])
            relay.own_y(chunks[UP])
            begin_y(chunks[DOWN])

    loads[spot.keys].wait()
    loads[spot.values].wait()
    loads[spot.up].wait()
    loads[spot.down].wait()
    loop(images, embed, "embed")
    canvas_out = pltpu.make_async_copy(v.canvas_v, canvas_hbm, v.store.at[images])
    canvas_out.start()
    relay.wait_y_all(chunks[QKV])

    def pair_copy(source, target, lane, recv, t_other):
        return pltpu.make_async_remote_copy(
            src_ref=source, dst_ref=target, send_sem=v.sent.at[lane], recv_sem=recv,
            device_id=(dp, t_other), device_id_type=MESH,
        )

    def near0(j):
        return pair_copy(v.near_out0.at[j], v.near_in0.at[j], 0, v.near0.at[j], near_t)

    def far0(j):
        return pair_copy(v.far_out0.at[j], v.far_in0.at[j], 1, v.far0.at[j], far_t)

    def near1(n, j, piece, turn):
        source, target = v.near_out1.at[n, j, :, piece], v.near_in1.at[n, j, :, piece]
        return pair_copy(source, target, 2, v.near1.at[n + turn, j], near_t)

    def far1(n, j, piece, turn):
        source, target = v.far_out1.at[n, j, :, piece], v.far_in1.at[n, j, :, piece]
        return pair_copy(source, target, 3, v.far1.at[n + turn, j], far_t)

    def swap2(j):
        return pair_copy(v.normed2.at[half + j], v.normed2.at[j], 4, v.swap2.at[j], near_t)

    def swap3(j):
        return pair_copy(v.normed3.at[half + j], v.normed3.at[j], 5, v.swap3.at[j], near_t)

    def attend(turn):
        slot = slot_of(turn)
        image = image_of(slot)

        @pl.when(turn == 2)
        def _():
            inside(True, lambda: relay.steps(up_late, 1))

        def project(tile):
            cols = pl.ds(pl.multiple_of(tile * heads_width, heads_width), heads_width)
            v.projected[:, cols] = dot(v.normed[slot], v.w_qkv[tile])

        loop(3, project)
        for head in range(head_total):
            low = head * head_size
            high = low + head_size
            query = (unit(v.projected[:, low:high]) * given.sharp[0, head]).astype(bf16)
            key_new = unit(v.projected[:, heads_width + low : heads_width + high]).astype(bf16)
            value_new = v.projected[:, 2 * heads_width + low : 2 * heads_width + high].astype(bf16)
            keys, values = v.all_keys.at[image, head], v.all_values.at[image, head]
            keys[:tokens, :] = key_new
            values[:tokens, :head_size] = value_new
            scores = dot_t(query, keys[...])
            weights = jnp.exp(scores - jnp.max(scores, axis=-1, keepdims=True)).astype(bf16)
            mixed = dot(weights, values[...])
            total = mixed[:, head_size : head_size + 1]
            v.attended[slot, :, low:high] = (mixed[:, :head_size] / total).astype(bf16)
            if head == 1:
                pl.when(turn == 0)(lambda: relay.cross_z(chunks[UP]))
                at_end(turn == 1, lambda: relay.steps(up_late, 0))

                @pl.when(turn == 1)
                def _():
                    relay.wait_y_all(chunks[OUT])
                    project_out(turn - 1)

        inside(turn == 0, lambda: relay.steps(up_late + up_early, 0))

        pl.when(turn > 0)(lambda: project_out(turn))

        at_end(turn == 1, lambda: relay.steps(up_early, 0))

        @pl.when(turn == 2)
        def _():
            inside(True, lambda: relay.steps(up_early, 1))
            relay.own_z(chunks[DOWN])
            relay.cross_z(chunks[DOWN])
            inside(True, lambda: relay.own_y(chunks[DOWN]))
            at_end(True, lambda: relay.steps(up_late, 1))
            at_end(True, lambda: relay.own_y(chunks[DOWN][:3]))

    def slot_of(turn):
        return turn // 2 + half * lax.rem(turn, 2)

    def project_out(turn):
        slot = slot_of(turn)
        image = image_of(slot)

        @pl.when(slot >= half)
        def _():
            near0(slot - half).wait_recv()

        def out_tile(tile):
            cols = pl.ds(pl.multiple_of(tile * block, block), block)
            partial = dot_t(v.attended[slot], v.w_out[cols, :])

            @pl.when(slot < half)
            def _():
                v.near_out0[slot, :, cols] = partial.astype(bf16)

            @pl.when(slot >= half)
            def _():
                pair = partial + v.near_in0[slot - half, :, cols].astype(f32)
                v.far_out0[slot - half, :, cols] = pair.astype(bf16)
                v.stream[slot - half, :, cols] += factor(0, image, cols) * pair

        loop(blocks, out_tile)
        pl.when(slot < half)(lambda: near0(slot).start())
        pl.when(slot >= half)(lambda: far0(slot - half).start())

    loop(images, attend, "attend")

    def second_norm(j):
        image = image_of(half + j)
        v.gain[j] = factor(1, image)
        far0(j).wait_recv()
        stream = v.stream[j] + factor(0, image) * v.far_in0[j].astype(f32)
        v.stream[j] = stream
        v.normed2[half + j] = modulate(stream, factor(3, image), factor(5, image)).astype(bf16)
        swap2(j).start()

    def second_norms(j):
        second_norm(j)

        @pl.when(j == 0)
        def _():
            at_end(True, lambda: relay.steps(up_early, 1))
            relay.steps(up_late, 2)
            at_end(True, lambda: relay.own_y(chunks[DOWN][3:]))
            inside(True, lambda: relay.steps(chunks[DOWN], 0))
            relay.steps(up_early, 2)

    loop(half, second_norms, "second_norm")
    relay.wait_y_all(chunks[UP])

    both = jnp.minimum(o, outer - 1 - o)
    sign = jnp.where(o < outer - 1 - o, 1, -1)

    def block_of(n):
        if blocks != outer:
            return n
        distance = (n + 1) // 2
        beside = o + distance * (1 - 2 * lax.rem(n, 2))
        beyond = o + sign * (n - both)
        return jnp.where(n <= 2 * both, beside, beyond)

    def wait_down(n, parts):
        if blocks == outer:
            for chunk in parts:
                if not relay.crosses_early(chunk):
                    relay.wait_y(chunk, block_of(n))

    def down_piece(n, low, size, first_j=0, count=half):
        start = block_of(n) * block + low
        cols = pl.ds(pl.multiple_of(start, 128), size)
        piece = slice(low, low + size)
        turn = low // size

        def theirs(j):
            v.near_out1[n, j, :, piece] = dot_t(v.hidden[j], v.w_down[cols, :]).astype(bf16)
            near1(n, j, piece, turn).start()

        loop(count, lambda j: theirs(first_j + j))

        def ours(j):
            partial = dot_t(v.hidden[half + j], v.w_down[cols, :])
            near1(n, j, piece, turn).wait_recv()
            pair = partial + v.near_in1[n, j, :, piece].astype(f32)
            v.far_out1[n, j, :, piece] = pair.astype(bf16)
            far1(n, j, piece, turn).start()
            v.stream[j, :, cols] += v.gain[j, :, cols] * pair

        loop(count, lambda j: ours(first_j + j))

    def add_far(n, j, low, size):
        start = block_of(n) * block + low
        cols = pl.ds(pl.multiple_of(start, 128), size)
        piece = slice(low, low + size)
        far1(n, j, piece, low // size).wait_recv()
        v.stream[j, :, cols] += v.gain[j, :, cols] * v.far_in1[n, j, :, piece].astype(f32)

    unit_tile = 512

    def lift_units(turn):
        slot = turn // 2 + half * (1 - lax.rem(turn, 2))
        pl.when(slot < half)(lambda: swap2(slot).wait_recv())

        def tile_units(tile):
            cols = pl.ds(pl.multiple_of(tile * unit_tile, unit_tile), unit_tile)
            lifted = dot(v.normed2[slot], v.w_up[:, cols])
            v.hidden[slot, :, cols] = jax.nn.gelu(lifted, approximate=True).astype(bf16)

        loop(units // unit_tile, tile_units)
        at_end(turn == 1, lambda: relay.steps(chunks[DOWN], 0))
        inside(turn == 1, lambda: relay.steps(chunks[DOWN], 1))
        if blocks == outer:

            @pl.when(lax.rem(turn, 2) == 1)
            def _():
                pl.when(turn == 1)(lambda: wait_down(0, chunks[DOWN]))
                down_piece(0, 0, block, turn // 2, 1)


    loop(images, lift_units, "lift_units")

    if blocks != outer:
        at_end(True, lambda: relay.steps(chunks[DOWN], 1))
        relay.steps(chunks[DOWN], 2)
        relay.wait_y_all(chunks[DOWN])

    most = 2 * len(chunks[DOWN]) // 3
    front, back = chunks[DOWN][:most], chunks[DOWN][most:]
    end = blocks - 1
    skip = 1 if blocks == outer else 0
    part = block // 3

    def down_relays(n, group):
        if blocks == outer:
            at_end(n == 1, lambda: relay.steps(group, 1))
            pl.when(n == 2)(lambda: relay.steps(group, 2))

    def down_block(n):
        n = n + skip
        down_relays(n, chunks[DOWN][:3])
        with jax.named_scope("wait_down"):
            wait_down(n, chunks[DOWN])
        down_piece(n, 0, block)
        down_relays(n, chunks[DOWN][3:])

        @pl.when(n > 1)
        def _():
            loop(half, lambda j: add_far(n - 2, j, 0, block))

    loop(end - skip, down_block, "down_block")
    with jax.named_scope("last_wait"):
        wait_down(end, front)
    down_piece(end, 0, part)
    down_piece(end, 2 * part, part)
    with jax.named_scope("last_wait"):
        wait_down(end, back)
    down_piece(end, part, part)
    loop(half, lambda j: add_far(end - 2, j, 0, block))
    loop(half, lambda j: add_far(end - 1, j, 0, block))
    with jax.named_scope("drain"):
        relay.drain()
    loads[spot.head_factors].wait()
    loads[spot.vocab].wait()

    def last_norm(j):
        image = image_of(half + j)
        for low in (0, 2 * part, part):
            add_far(end, j, low, part)
        factors = v.s_head_factors.at[image]
        v.normed3[half + j] = modulate(
            v.stream[j], factors[0:1, :], factors[1:2, :]
        ).astype(bf16)
        swap3(j).start()

    loop(half, last_norm, "last_norm")

    def logits_out(image):
        return pltpu.make_async_copy(
            v.logits_v.at[image], logits_hbm.at[image], v.store.at[image]
        )

    def give_logits(turn):
        slot = lax.rem(turn + half, images)
        image = image_of(slot)
        pl.when(slot < half)(lambda: swap3(slot).wait_recv())
        v.logits_v[image] = dot(v.normed3[slot], v.s_vocab[...]).astype(bf16)
        logits_out(image).start()

    loop(images, give_logits, "give_logits")

    for lane, source in enumerate(
        (
            v.near_out0, v.far_out0, v.near_out1, v.far_out1,
            v.normed2.at[pl.ds(half, half)], v.normed3.at[pl.ds(half, half)],
        )
    ):
        relay.wait(source, send=v.sent.at[lane])
    loop(images, lambda image: logits_out(image).wait())
    canvas_out.wait()


def local(
    dp_total, tensor_total, ids, codes, summed, lift, offset, factors, sharp, qkv, out, up, down,
    keys, values, head_factors, vocab,
):
    images, prev = ids.shape
    tokens, width = offset.shape
    rows = qkv.shape[1]
    outer = dp_total // 2
    group = 1
    while (2 * rows * group) % 128:
        group *= 2
    heads_width = out.shape[1]
    assert tensor_total == 4 and images % 2 == 0 and dp_total % 2 == 0
    down_parts = 6 if rows % 96 == 0 else 3
    dims = SimpleNamespace(
        outer=outer, rows=rows, images=images, tokens=tokens, width=width,
        heads_width=heads_width, heads=sharp.shape[1], units=up.shape[2],
        prev=prev, channels=codes.shape[1], codes=codes.shape[0],
        vocab=vocab.shape[1], cache=keys.shape[2], half=images // 2,
        blocks=outer // group, parts=(3, 1, 3, down_parts), early=EARLY,
    )
    grow = interp_matrix(SIDE, PREV)
    grow = jnp.asarray(np.kron(grow, grow), f32)
    given = (
        ids, codes.T, summed.swapaxes(1, 2), lift, offset, factors[0].swapaxes(0, 1), sharp,
        qkv[0].swapaxes(0, 1), out[0].T, up[0], down[0].T, keys[0], values[0],
        head_factors, vocab, grow,
    )
    anywhere = pl.BlockSpec(memory_space=pl.ANY)
    specs = [anywhere] * len(INPUTS)
    specs[Given(*range(len(INPUTS))).sharp] = pl.BlockSpec(memory_space=pltpu.SMEM)
    logits, canvas = pl.pallas_call(
        functools.partial(step_kernel, dims),
        out_shape=(
            jax.ShapeDtypeStruct((images, tokens, vocab.shape[1]), bf16),
            jax.ShapeDtypeStruct((images, summed.shape[2], tokens), f32),
        ),
        in_specs=specs,
        out_specs=(anywhere, anywhere),
        scratch_shapes=list(scratch_shapes(dims).values()),
        compiler_params=pltpu.CompilerParams(
            collective_id=0, has_side_effects=True, vmem_limit_bytes=67043328
        ),
        name="step",
    )(*given)
    return logits, canvas.swapaxes(1, 2)


def solution(mesh):
    placed = (
        P("dp", None),
        P(),
        P("dp", None, None),
        P(),
        P(),
        P(None, "dp", None, None),
        P(None, "tensor"),
        P(None, "dp", None, "tensor"),
        P(None, "tensor", "dp"),
        P(None, "dp", "tensor"),
        P(None, "tensor", "dp"),
        P(None, "dp", None, "tensor"),
        P(None, "dp", None, "tensor"),
        P("dp", None, None),
        P(None, "tensor"),
    )
    return jax.shard_map(
        functools.partial(local, mesh.shape["dp"], mesh.shape["tensor"]),
        mesh=mesh,
        in_specs=placed,
        out_specs=(P("dp", None, "tensor"), P("dp", None, None)),
        check_vma=False,
    )
```
